128 devices in a mesh: row: 16 (over x, z), col: 8 (over y, core).
Axes of the slice: x: 4, y: 4, z: 4, core: 2. Of those that a mesh axis runs over, the one named last changes fastest.
Arguments:
- front_pivot: float32 [128, 128, 128], P('col', 'row'), may hold values from -256 to 256, as said below
- front_update: float32 [128, 640, 768], P('col', 'row'), may hold values from -12 to 12, as said below
- child_blocks: float32 [128, 2, 512, 512], P('col', None, 'row'), may hold values from -0.5 to 0.5, as said below
- child_map: int32 [128, 2, 512], P('col'), may hold values from -1 to 767, as said below
Outputs:
- lhat: float32 [128, 640, 128], P('col', 'row')
- schur: float32 [128, 640, 640], P('col', 'row')
- negative_share: float32 [], replicated
The draws below stay inside these ranges and needn't reach their ends.
Inputs may be any that keep to these rules, and one draw needn't show every extreme that they name: `front_pivot`: symmetric in its last two dimensions. With both children's entries added, the pivot block of every front has an LDL^T factorization without pivoting whose pivots have magnitudes 4 to 40. `front_update`: the last 640 columns of each front form a symmetric matrix. `child_blocks`: symmetric in its last two dimensions. child_map[f, c, i] is the row and column of front f's assembled matrix that row and column i of child c go to, or -1 for padding. A child's entries of 0 or more are distinct, come before its padding, and number at least 385, and more than half of 512. Parent row p is held by grid row p // 8 if p < 128, else by (p - 128) // 40. Of the 32 rows i of a child with the same i // 32, at most 4 go to rows held by any one grid row, and every child reaches that bound.
All inputs are finite; a program needn't handle non-finite values.
Results may differ from the reference program's by a relative error of at most 0.0003.
Values sent between devices are 32-bit elements; how exact they have to be, the bound alone decides.
A program may use at most 64 MiB of HBM per device.

```python
import jax
import jax.numpy as jnp
from jax import lax

F = 768
S = 128
CU = 512
U = 640
NFRONT = 128
SP = 8
UP = 40
HELD = 32
CAP = 4
N_ROW = 16


def draw_front_pivot(key, part):
    key_list = jax.random.split(jax.random.fold_in(key, 11), 3)
    reach = 1.2 * (3.0 / S) ** 0.5
    entries = jax.random.uniform(key_list[0], (NFRONT, S, S), jnp.float32, -reach, reach)
    index = jnp.arange(S, dtype=jnp.int32)
    strict = index[:, None] > index[None, :]
    unit_factor = jnp.where(strict[None, :, :], entries, jnp.zeros_like(entries)) + jnp.eye(S, dtype=jnp.float32)[None, :, :]
    logs = jax.random.uniform(key_list[1], (NFRONT, S), jnp.float32, jnp.log(4.0), jnp.log(40.0))
    magnitude = jnp.exp(logs)
    neg_rate = 0.15 + 0.45 * jnp.arange(NFRONT, dtype=jnp.float32) / max(NFRONT - 1, 1)
    negative = jax.random.uniform(key_list[2], (NFRONT, S), jnp.float32) < neg_rate[:, None]
    pivots = jnp.where(negative, -magnitude, magnitude)
    target = jnp.einsum('fik,fjk->fij', unit_factor * pivots[:, None, :], unit_factor, precision=lax.Precision.HIGHEST)
    target = 0.5 * (target + jnp.swapaxes(target, 1, 2))
    blocks = draw_child_blocks(key, part)
    maps = draw_child_map(key, part)
    slots = jnp.arange(S, dtype=jnp.int32)
    hot = (maps[:, :, None, :] == slots[None, None, :, None]).astype(jnp.float32)
    spread = jnp.einsum('fcpi,fcij->fcpj', hot, blocks, precision=lax.Precision.HIGHEST)
    added = jnp.einsum('fcpj,fcqj->fpq', spread, hot, precision=lax.Precision.HIGHEST)
    return (target - added).astype(jnp.float32)


def draw_front_update(key, part):
    key_list = jax.random.split(jax.random.fold_in(key, 23), 1)
    values = jnp.clip(2.0 * jax.random.normal(key_list[0], (NFRONT, U, F), jnp.float32), -8.0, 8.0)
    coupling = values[:, :, :S]
    trailing = values[:, :, S:]
    trailing = (trailing + jnp.swapaxes(trailing, 1, 2)) * 0.7071
    return jnp.concatenate([coupling, trailing], axis=2).astype(jnp.float32)


def draw_child_blocks(key, part):
    key_list = jax.random.split(jax.random.fold_in(key, 31), 1)
    random_part = jax.random.uniform(key_list[0], (NFRONT, 2, CU, CU), jnp.float32, -0.5, 0.5)
    return (0.5 * (random_part + jnp.swapaxes(random_part, 2, 3))).astype(jnp.float32)


def draw_child_map(key, part):
    lowest = max(CU - 127, CU // 2 + 1)

    def one_child(child_key):
        key_list = jax.random.split(child_key, 3)
        count = jax.random.randint(key_list[0], (), lowest, CU + 1)
        offsets = jax.random.permutation(key_list[1], N_ROW)[:N_ROW // 2]
        targets = jax.vmap(lambda inner: jax.random.permutation(inner, SP + UP)[:HELD])(jax.random.split(key_list[2], N_ROW))
        position = jnp.arange(CU, dtype=jnp.int32)
        source = position // HELD
        within = position % HELD
        group = within // CAP
        owner = (source + offsets[group]) % N_ROW
        local = targets[owner, within]
        parent = jnp.where(local < SP, owner * SP + local, S + owner * UP + local - SP)
        return jnp.where(position < count, parent, -1).astype(jnp.int32)
    key_list = jax.random.split(jax.random.fold_in(key, 37), NFRONT * 2)
    return jax.vmap(one_child)(key_list).reshape(NFRONT, 2, CU).astype(jnp.int32)


def setup_inputs(seed: int = 0) -> dict:
    keys = jax.random.split(jax.random.key(seed), 5)
    front_pivot = draw_front_pivot(jax.random.fold_in(keys[4], 71), 0)
    front_update = draw_front_update(jax.random.fold_in(keys[4], 71), 0)
    child_blocks = draw_child_blocks(jax.random.fold_in(keys[4], 71), 0)
    child_map = draw_child_map(jax.random.fold_in(keys[4], 71), 0)
    return {"front_pivot": front_pivot, "front_update": front_update, "child_blocks": child_blocks, "child_map": child_map}


highest = lax.Precision.HIGHEST

def factor(blocks):
    count = blocks.shape[-1]
    index = jnp.arange(count, dtype=jnp.int32)

    def eliminate(column_index, carry):
        current, pivots = carry
        column = lax.dynamic_index_in_dim(current, column_index, 2, keepdims=False)
        leading = lax.dynamic_index_in_dim(current, column_index, 1, keepdims=False)
        pivot = lax.dynamic_index_in_dim(column, column_index, 1, keepdims=False)
        below = index[None, :] > column_index
        multiplier = jnp.where(below, column / pivot[:, None], jnp.zeros_like(column))
        current = current - multiplier[:, :, None] * leading[:, None, :]
        pivots = jnp.where(index[None, :] == column_index, pivot[:, None], pivots)
        return (current, pivots)
    start = (blocks, jnp.zeros(blocks.shape[:2], blocks.dtype))
    current, pivots = lax.fori_loop(0, count, eliminate, start)
    upper = jnp.where(index[:, None] <= index[None, :], current, jnp.zeros_like(current)) / pivots[:, :, None]
    lower = jnp.swapaxes(upper, 1, 2)
    identity = jnp.eye(count, dtype=blocks.dtype)
    inverse = jax.vmap(lambda matrix: jax.scipy.linalg.solve_triangular(matrix, identity, lower=True, unit_diagonal=True))(lower)
    return (inverse, pivots)

def assemble(inputs):
    pivot_rows, update_rows, blocks, indices = inputs
    upper_rows = jnp.concatenate([pivot_rows, jnp.swapaxes(update_rows[:, :S], 0, 1)], axis=1)
    whole = jnp.concatenate([upper_rows, update_rows], axis=0)
    for child in range(2):
        spot = jnp.where(indices[child] >= 0, indices[child], F).astype(jnp.int32)
        whole = whole.at[spot[:, None], spot[None, :]].add(blocks[child], mode='drop')
    return (whole[:S, :S], whole[S:, :S], whole[S:, S:])

def reference(front_pivot, front_update, child_blocks, child_map):
    pivot_block, coupling, trailing = lax.map(assemble, (front_pivot, front_update, child_blocks, child_map))
    inverse, pivots = factor(pivot_block)
    lhat = jnp.einsum('fik,fjk->fij', coupling, inverse, precision=highest)
    scaled = lhat / pivots[:, None, :]
    schur = trailing - jnp.einsum('fik,fjk->fij', scaled, lhat, precision=highest)
    negatives = jnp.sum(jnp.where(pivots < 0.0, 1.0, 0.0).astype(jnp.float32))
    negative_share = (negatives / (NFRONT * S)).astype(jnp.float32)
    return (lhat, schur, negative_share)
```

```python
import functools

import jax
import jax.numpy as jnp
from jax import lax
from jax.experimental import pallas as pl
from jax.experimental.pallas import tpu as pltpu
from jax.sharding import PartitionSpec as P

MESH = pl.DeviceIdType.MESH
F32 = jnp.float32
BF16 = jnp.bfloat16
HIGHEST = lax.Precision.HIGHEST

N_ROW = 16
N_COL = 8
SIDE = 4
S = 128
CU = 512
U = 640
F = 768
SP = 8
UP = 40
HELD = 32
OFFSETS = [(dx, dz) for dx in range(SIDE) for dz in range(SIDE) if (dx, dz) != (0, 0)]


def peer(me, dx, dz):
    x = lax.rem(me // SIDE + dx, SIDE)
    z = lax.rem(lax.rem(me, SIDE) + dz, SIDE)
    return x * SIDE + z


def greet(row_peers, col_peers):
    barrier = pltpu.get_barrier_semaphore()
    for other in row_peers:
        pl.semaphore_signal(barrier, inc=1, device_id={"row": other}, device_id_type=MESH)
    for other in col_peers:
        pl.semaphore_signal(barrier, inc=1, device_id={"col": other}, device_id_type=MESH)
    pl.semaphore_wait(barrier, len(row_peers) + len(col_peers))


def gather_kernel(
    child_ref, pivot_ref, update_ref, near_ref, next_ref, far_ref, panel_ref, send_sem, recv_sem, own_sem
):
    me = lax.axis_index("row")
    group = me // SIDE
    near = pl.multiple_of(group * 128, 128)
    following = pl.multiple_of(lax.rem(group + 1, 4) * 128, 128)
    opposite = pl.multiple_of(lax.rem(group + 2, 4) * 128, 128)
    far_child = group // 2
    rows = pl.ds(pl.multiple_of(me * HELD, HELD), HELD)
    pivot_rows = pl.ds(pl.multiple_of(me * SP, SP), SP)
    update_rows = pl.ds(pl.multiple_of(S + me * UP, SP), UP)

    def pieces(front):
        return (
            (pivot_ref.at[front], panel_ref.at[pivot_rows]),
            (child_ref.at[front, :, :, pl.ds(near, 128)], near_ref.at[:, rows]),
            (child_ref.at[front, :, :, pl.ds(following, 128)], next_ref.at[:, rows]),
            (child_ref.at[front, far_child, :, pl.ds(opposite, 128)], far_ref.at[rows]),
            (update_ref.at[front, :, pl.ds(0, S)], panel_ref.at[update_rows]),
        )

    own = [
        pltpu.make_async_copy(source, target, own_sem.at[i])
        for i, (source, target) in enumerate(pieces(me))
    ]
    for copy in own:
        copy.start()
    others = [peer(me, dx, dz) for dx, dz in OFFSETS]
    greet(others, [])
    copies = []
    for place, other in enumerate(others):
        for i, (source, target) in enumerate(pieces(other)):
            copies.append(
                pltpu.make_async_remote_copy(
                    src_ref=source,
                    dst_ref=target,
                    send_sem=send_sem.at[place, i],
                    recv_sem=recv_sem.at[place, i],
                    device_id={"row": other},
                    device_id_type=MESH,
                )
            )
            copies[-1].start()
    for copy in own:
        copy.wait()
    for copy in copies:
        copy.wait()


def gather(child_blocks, front_pivot, front_update):
    any_spec = pl.BlockSpec(memory_space=pl.ANY)
    vmem_spec = pl.BlockSpec(memory_space=pltpu.VMEM)
    return pl.pallas_call(
        gather_kernel,
        out_shape=(
            jax.ShapeDtypeStruct((2, CU, 128), F32),
            jax.ShapeDtypeStruct((2, CU, 128), F32),
            jax.ShapeDtypeStruct((CU, 128), F32),
            jax.ShapeDtypeStruct((F, S), F32),
        ),
        in_specs=[any_spec] * 3,
        out_specs=(vmem_spec,) * 4,
        scratch_shapes=[
            pltpu.SemaphoreType.DMA((len(OFFSETS), 5)),
            pltpu.SemaphoreType.DMA((len(OFFSETS), 5)),
            pltpu.SemaphoreType.DMA((5,)),
        ],
        compiler_params=pltpu.CompilerParams(collective_id=0, has_side_effects=True),
        name="gather_fronts",
    )(child_blocks, front_pivot, front_update)


def split(values):
    high = values.astype(BF16)
    low = (values - high.astype(F32)).astype(BF16)
    return high, low


def nt_dot(a, b, precision=None):
    return lax.dot_general(
        a, b, (((1,), (1,)), ((), ())), precision=precision, preferred_element_type=F32
    )


BLOCK = 32


def factor_in_place(work):
    sub = lax.broadcasted_iota(jnp.int32, (8, 128), 0)
    groups = BLOCK // 8
    for block in range(S // BLOCK):
        base = block * BLOCK
        left = [work[base + 8 * g : base + 8 * g + 8, 0:128] for g in range(groups)]
        right = [work[base + 8 * g : base + 8 * g + 8, 128:256] for g in range(groups)]
        for step in range(BLOCK):
            k = base + step
            own, inner = step // 8, step % 8
            row_left = jnp.broadcast_to(left[own][inner : inner + 1, :], (8, 128))
            row_right = jnp.broadcast_to(right[own][inner : inner + 1, :], (8, 128))
            pivot = jnp.broadcast_to(row_left[:, k : k + 1], (8, 128))
            scale = 1.0 / pivot
            for g in range(own, groups):
                column = jnp.broadcast_to(left[g][:, k : k + 1], (8, 128))
                multiplier = column * scale
                if g == own:
                    multiplier = jnp.where(sub > inner, multiplier, 0.0)
                left[g] = left[g] - multiplier * row_left
                right[g] = right[g] - multiplier * row_right
        strip_left = jnp.concatenate(left, axis=0)
        strip_right = jnp.concatenate(right, axis=0)
        work[base : base + BLOCK, 0:128] = strip_left
        work[base : base + BLOCK, 128:256] = strip_right
        after = base + BLOCK
        if after < S:
            lanes = lax.broadcasted_iota(jnp.int32, (BLOCK, 128), 1)
            places = lax.broadcasted_iota(jnp.int32, (BLOCK, 128), 0) + base
            diagonal = jnp.sum(
                jnp.where(lanes == places, strip_left, 0.0), axis=1, keepdims=True
            )
            lower = strip_left / diagonal
            strip = jnp.concatenate([strip_left, strip_right], axis=1)
            product = lax.dot_general(
                lower, strip, (((0,), (0,)), ((), ())), precision=HIGHEST, preferred_element_type=F32
            )
            work[after:S, :] = work[after:S, :] - product[after:S, :]


def front_kernel(
    map_ref, near_ref, next_ref, far_ref, panel_ref, lhat_ref, rest_ref, negative_ref, hot_ref, work, high_ref, low_ref
):
    me = lax.axis_index("row")
    for child in range(2):
        indices = map_ref[me, child : child + 1, :]
        position = lax.broadcasted_iota(jnp.int32, (F, CU), 0)
        hot_ref[child] = jnp.where(indices == position, 1.0, 0.0).astype(BF16)

    def fill(child, i, j, block):
        high, low = split(block)
        high_ref[child, 128 * i : 128 * i + 128, 128 * j : 128 * j + 128] = high
        low_ref[child, 128 * i : 128 * i + 128, 128 * j : 128 * j + 128] = low

    for child in range(2):
        for i in range(4):
            rows = slice(128 * i, 128 * i + 128)
            fill(child, i, i, near_ref[child, rows, :])
            block = next_ref[child, rows, :]
            fill(child, i, (i + 1) % 4, block)
            fill(child, (i + 1) % 4, i, block.T)
    for i in range(4):
        child = i // 2
        block = far_ref[128 * i : 128 * i + 128, :]
        fill(child, i, (i + 2) % 4, block)
        fill(child, (i + 2) % 4, i, block.T)

    spread = []
    for child in range(2):
        hot = hot_ref[child]
        high = jnp.dot(hot, high_ref[child], preferred_element_type=F32).astype(BF16)
        low = jnp.dot(hot, low_ref[child], preferred_element_type=F32).astype(BF16)
        spread.append((high, low))

    def columns(start, size, first=0):
        total = None
        for child in range(2):
            hot = hot_ref[child, start : start + size, :]
            for part in spread[child]:
                term = nt_dot(part[first:, :], hot)
                total = term if total is None else total + term
        return total

    panel = panel_ref[...] + columns(0, S)
    lane = lax.broadcasted_iota(jnp.int32, (S, S), 1)
    place = lax.broadcasted_iota(jnp.int32, (S, S), 0)
    work[:, 0:128] = panel[:S]
    work[:, 128:256] = jnp.where(lane == place, 1.0, 0.0)
    factor_in_place(work)
    inverse = work[:, 128:256]
    pivots = jnp.sum(jnp.where(lane == place, work[:, 0:128], 0.0), axis=0, keepdims=True)
    negative_ref[0] = jnp.where(pivots < 0.0, 1.0, 0.0)
    lhat = nt_dot(panel[S:], inverse, HIGHEST)
    lhat_ref[...] = lhat
    scaled = lhat / pivots
    for start in range(0, U, 128):
        correction = nt_dot(scaled, lhat[start : start + 128], HIGHEST)
        rest_ref[:, start : start + 128] = columns(S + start, 128, S) - correction


def front(child_map, near, following, far, panel):
    vmem_spec = pl.BlockSpec(memory_space=pltpu.VMEM)
    return pl.pallas_call(
        front_kernel,
        out_shape=(
            jax.ShapeDtypeStruct((U, S), F32),
            jax.ShapeDtypeStruct((U, U), F32),
            jax.ShapeDtypeStruct((1, 1, S), F32),
        ),
        in_specs=[vmem_spec] * 5,
        out_specs=(vmem_spec,) * 3,
        scratch_shapes=[
            pltpu.VMEM((2, F, CU), BF16),
            pltpu.VMEM((S, 2 * S), F32),
            pltpu.VMEM((2, CU, CU), BF16),
            pltpu.VMEM((2, CU, CU), BF16),
        ],
        name="front_factor",
    )(child_map, near, following, far, panel)


def scatter_kernel(
    lhat_ref, rest_ref, negative_ref, lhat_out, rest_out, share_out,
    counts, send_sem, recv_sem, count_send, count_recv, row_send, row_recv, own_sem
):
    me = lax.axis_index("row")
    col = lax.axis_index("col")
    others = [peer(me, dx, dz) for dx, dz in OFFSETS]
    columns = [lax.rem(col + d, N_COL) for d in range(1, N_COL)]

    def rows(row):
        return pl.ds(pl.multiple_of(row * UP, SP), UP)

    own = [
        pltpu.make_async_copy(negative_ref, counts.at[me, pl.ds(col, 1)], own_sem.at[0]),
        pltpu.make_async_copy(lhat_ref.at[rows(me)], lhat_out.at[me], own_sem.at[1]),
        pltpu.make_async_copy(rest_ref.at[rows(me)], rest_out.at[me], own_sem.at[2]),
    ]
    for copy in own:
        copy.start()
    greet(others, columns)
    tallies = []
    for place, other in enumerate(columns):
        tallies.append(
            pltpu.make_async_remote_copy(
                src_ref=negative_ref,
                dst_ref=counts.at[me, pl.ds(col, 1)],
                send_sem=count_send.at[place],
                recv_sem=count_recv.at[place],
                device_id={"col": other},
                device_id_type=MESH,
            )
        )
        tallies[-1].start()
    copies = []
    for place, other in enumerate(others):
        for i, (source, target) in enumerate(((lhat_ref, lhat_out), (rest_ref, rest_out))):
            copies.append(
                pltpu.make_async_remote_copy(
                    src_ref=source.at[rows(other)],
                    dst_ref=target.at[me],
                    send_sem=send_sem.at[place, i],
                    recv_sem=recv_sem.at[place, i],
                    device_id={"row": other},
                    device_id_type=MESH,
                )
            )
            copies[-1].start()
    for copy in own:
        copy.wait()
    for copy in tallies:
        copy.wait()
    forwards = []
    for place, other in enumerate(others):
        forwards.append(
            pltpu.make_async_remote_copy(
                src_ref=counts.at[me],
                dst_ref=counts.at[me],
                send_sem=row_send.at[place],
                recv_sem=row_recv.at[place],
                device_id={"row": other},
                device_id_type=MESH,
            )
        )
        forwards[-1].start()
    for copy in copies:
        copy.wait()
    for copy in forwards:
        copy.wait()
    total = counts[0]
    for row in range(1, N_ROW):
        total = total + counts[row]
    flat = jnp.sum(total, axis=0)
    share_out[...] = jnp.sum(flat, axis=1, keepdims=True) / float(N_ROW * N_COL * S)


def scatter(lhat, rest, negative):
    any_spec = pl.BlockSpec(memory_space=pl.ANY)
    vmem_spec = pl.BlockSpec(memory_space=pltpu.VMEM)
    count = len(OFFSETS)
    return pl.pallas_call(
        scatter_kernel,
        out_shape=(
            jax.ShapeDtypeStruct((N_ROW, UP, S), F32),
            jax.ShapeDtypeStruct((N_ROW, UP, U), F32),
            jax.ShapeDtypeStruct((1, 1), F32),
        ),
        in_specs=[any_spec] * 3,
        out_specs=(vmem_spec,) * 3,
        scratch_shapes=[
            pltpu.VMEM((N_ROW, N_COL, 1, S), F32),
            pltpu.SemaphoreType.DMA((count, 2)),
            pltpu.SemaphoreType.DMA((count, 2)),
            pltpu.SemaphoreType.DMA((N_COL - 1,)),
            pltpu.SemaphoreType.DMA((N_COL - 1,)),
            pltpu.SemaphoreType.DMA((count,)),
            pltpu.SemaphoreType.DMA((count,)),
            pltpu.SemaphoreType.DMA((3,)),
        ],
        compiler_params=pltpu.CompilerParams(collective_id=1, has_side_effects=True),
        name="scatter_fronts",
    )(lhat, rest, negative)


def local(front_pivot, front_update, child_blocks, child_map):
    near, following, far, panel = gather(child_blocks, front_pivot, front_update)
    lhat, rest, negative = front(child_map, near, following, far, panel)
    lhat, rest, share = scatter(lhat, rest, negative)
    return (lhat, front_update[:, :, S:] + rest, share[0, 0])


def solution(mesh):
    in_specs = (
        P("col", "row", None),
        P("col", "row", None),
        P("col", None, "row", None),
        P("col", None, None),
    )
    out_specs = (P("col", "row", None), P("col", "row", None), P())
    return jax.shard_map(local, mesh=mesh, in_specs=in_specs, out_specs=out_specs, check_vma=False)
```

```python
import functools

import jax
import jax.numpy as jnp
from jax import lax
from jax.experimental import pallas as pl
from jax.experimental.pallas import tpu as pltpu
from jax.sharding import PartitionSpec as P

MESH = pl.DeviceIdType.MESH
F32 = jnp.float32
BF16 = jnp.bfloat16
HIGHEST = lax.Precision.HIGHEST

N_ROW = 16
N_COL = 8
SIDE = 4
S = 128
CU = 512
U = 640
F = 768
SP = 8
UP = 40
HELD = 32
OFFSETS = [
    (dx, (dx + turn) % SIDE)
    for turn in range(SIDE)
    for dx in range(SIDE)
    if (dx, (dx + turn) % SIDE) != (0, 0)
]


def peer(me, dx, dz):
    x = lax.rem(me // SIDE + dx, SIDE)
    z = lax.rem(lax.rem(me, SIDE) + dz, SIDE)
    return x * SIDE + z


def greet(row_peers, col_peers):
    barrier = pltpu.get_barrier_semaphore()
    for other in row_peers:
        pl.semaphore_signal(barrier, inc=1, device_id={"row": other}, device_id_type=MESH)
    for other in col_peers:
        pl.semaphore_signal(barrier, inc=1, device_id={"col": other}, device_id_type=MESH)
    pl.semaphore_wait(barrier, len(row_peers) + len(col_peers))


def gather_kernel(
    child_ref, pivot_ref, update_ref, near_ref, next_ref, far_ref, panel_ref, send_sem, recv_sem, own_sem
):
    me = lax.axis_index("row")
    group = me // SIDE
    near = pl.multiple_of(group * 128, 128)
    following = pl.multiple_of(lax.rem(group + 1, 4) * 128, 128)
    opposite = pl.multiple_of(lax.rem(group + 2, 4) * 128, 128)
    far_child = group // 2
    rows = pl.ds(pl.multiple_of(me * HELD, HELD), HELD)
    pivot_rows = pl.ds(pl.multiple_of(me * SP, SP), SP)
    update_rows = pl.ds(pl.multiple_of(S + me * UP, SP), UP)

    def pieces(front):
        return (
            (pivot_ref.at[front], panel_ref.at[pivot_rows]),
            (child_ref.at[front, :, :, pl.ds(near, 128)], near_ref.at[:, rows]),
            (child_ref.at[front, :, :, pl.ds(following, 128)], next_ref.at[:, rows]),
            (child_ref.at[front, far_child, :, pl.ds(opposite, 128)], far_ref.at[rows]),
            (update_ref.at[front, :, pl.ds(0, S)], panel_ref.at[update_rows]),
        )

    own = [
        pltpu.make_async_copy(source, target, own_sem.at[i])
        for i, (source, target) in enumerate(pieces(me))
    ]
    for copy in own:
        copy.start()
    others = [peer(me, dx, dz) for dx, dz in OFFSETS]
    greet(others, [])
    copies = []
    for place, other in enumerate(others):
        for i, (source, target) in enumerate(pieces(other)):
            copies.append(
                pltpu.make_async_remote_copy(
                    src_ref=source,
                    dst_ref=target,
                    send_sem=send_sem.at[place, i],
                    recv_sem=recv_sem.at[place, i],
                    device_id={"row": other},
                    device_id_type=MESH,
                )
            )
            copies[-1].start()
    for copy in own:
        copy.wait()
    for copy in copies:
        copy.wait()


def gather(child_blocks, front_pivot, front_update):
    any_spec = pl.BlockSpec(memory_space=pl.ANY)
    vmem_spec = pl.BlockSpec(memory_space=pltpu.VMEM)
    return pl.pallas_call(
        gather_kernel,
        out_shape=(
            jax.ShapeDtypeStruct((2, CU, 128), F32),
            jax.ShapeDtypeStruct((2, CU, 128), F32),
            jax.ShapeDtypeStruct((CU, 128), F32),
            jax.ShapeDtypeStruct((F, S), F32),
        ),
        in_specs=[any_spec] * 3,
        out_specs=(vmem_spec,) * 4,
        scratch_shapes=[
            pltpu.SemaphoreType.DMA((len(OFFSETS), 5)),
            pltpu.SemaphoreType.DMA((len(OFFSETS), 5)),
            pltpu.SemaphoreType.DMA((5,)),
        ],
        compiler_params=pltpu.CompilerParams(collective_id=0, has_side_effects=True),
        name="gather_fronts",
    )(child_blocks, front_pivot, front_update)


def split(values):
    high = values.astype(BF16)
    low = (values - high.astype(F32)).astype(BF16)
    return high, low


def nt_dot(a, b, precision=None):
    return lax.dot_general(
        a, b, (((1,), (1,)), ((), ())), precision=precision, preferred_element_type=F32
    )


BLOCK = 32


def factor_in_place(work):
    sub = lax.broadcasted_iota(jnp.int32, (8, 128), 0)
    groups = BLOCK // 8
    for block in range(S // BLOCK):
        base = block * BLOCK
        left = [work[base + 8 * g : base + 8 * g + 8, 0:128] for g in range(groups)]
        right = [work[base + 8 * g : base + 8 * g + 8, 128:256] for g in range(groups)]
        for step in range(BLOCK):
            k = base + step
            own, inner = step // 8, step % 8
            row_left = jnp.broadcast_to(left[own][inner : inner + 1, :], (8, 128))
            row_right = jnp.broadcast_to(right[own][inner : inner + 1, :], (8, 128))
            pivot = jnp.broadcast_to(row_left[:, k : k + 1], (8, 128))
            scale = 1.0 / pivot
            for g in range(own, groups):
                column = jnp.broadcast_to(left[g][:, k : k + 1], (8, 128))
                multiplier = column * scale
                if g == own:
                    multiplier = jnp.where(sub > inner, multiplier, 0.0)
                left[g] = left[g] - multiplier * row_left
                right[g] = right[g] - multiplier * row_right
        strip_left = jnp.concatenate(left, axis=0)
        strip_right = jnp.concatenate(right, axis=0)
        work[base : base + BLOCK, 0:128] = strip_left
        work[base : base + BLOCK, 128:256] = strip_right
        after = base + BLOCK
        if after < S:
            lanes = lax.broadcasted_iota(jnp.int32, (BLOCK, 128), 1)
            places = lax.broadcasted_iota(jnp.int32, (BLOCK, 128), 0) + base
            diagonal = jnp.sum(
                jnp.where(lanes == places, strip_left, 0.0), axis=1, keepdims=True
            )
            lower = strip_left / diagonal
            strip = jnp.concatenate([strip_left, strip_right], axis=1)
            product = lax.dot_general(
                lower, strip, (((0,), (0,)), ((), ())), precision=HIGHEST, preferred_element_type=F32
            )
            work[after:S, :] = work[after:S, :] - product[after:S, :]


def front_kernel(
    map_ref, near_ref, next_ref, far_ref, panel_ref, lhat_ref, rest_ref, negative_ref, hot_ref, work, high_ref, low_ref
):
    me = lax.axis_index("row")
    for child in range(2):
        indices = map_ref[me, child : child + 1, :]
        position = lax.broadcasted_iota(jnp.int32, (F, CU), 0)
        hot_ref[child] = jnp.where(indices == position, 1.0, 0.0).astype(BF16)

    def fill(child, i, j, block):
        high, low = split(block)
        high_ref[child, 128 * i : 128 * i + 128, 128 * j : 128 * j + 128] = high
        low_ref[child, 128 * i : 128 * i + 128, 128 * j : 128 * j + 128] = low

    for child in range(2):
        for i in range(4):
            rows = slice(128 * i, 128 * i + 128)
            fill(child, i, i, near_ref[child, rows, :])
            block = next_ref[child, rows, :]
            fill(child, i, (i + 1) % 4, block)
            fill(child, (i + 1) % 4, i, block.T)
    for i in range(4):
        child = i // 2
        block = far_ref[128 * i : 128 * i + 128, :]
        fill(child, i, (i + 2) % 4, block)
        fill(child, (i + 2) % 4, i, block.T)

    spread = []
    for child in range(2):
        hot = hot_ref[child]
        high = jnp.dot(hot, high_ref[child], preferred_element_type=F32).astype(BF16)
        low = jnp.dot(hot, low_ref[child], preferred_element_type=F32).astype(BF16)
        spread.append((high, low))

    def columns(start, size, first=0):
        total = None
        for child in range(2):
            hot = hot_ref[child, start : start + size, :]
            for part in spread[child]:
                term = nt_dot(part[first:, :], hot)
                total = term if total is None else total + term
        return total

    panel = panel_ref[...] + columns(0, S)
    lane = lax.broadcasted_iota(jnp.int32, (S, S), 1)
    place = lax.broadcasted_iota(jnp.int32, (S, S), 0)
    work[:, 0:128] = panel[:S]
    work[:, 128:256] = jnp.where(lane == place, 1.0, 0.0)
    factor_in_place(work)
    inverse = work[:, 128:256]
    pivots = jnp.sum(jnp.where(lane == place, work[:, 0:128], 0.0), axis=0, keepdims=True)
    negative_ref[0] = jnp.where(pivots < 0.0, 1.0, 0.0)
    lhat = nt_dot(panel[S:], inverse, HIGHEST)
    lhat_ref[...] = lhat
    scaled = lhat / pivots
    for start in range(0, U, 128):
        correction = nt_dot(scaled, lhat[start : start + 128], HIGHEST)
        rest_ref[:, start : start + 128] = columns(S + start, 128, S) - correction


def front(child_map, near, following, far, panel):
    vmem_spec = pl.BlockSpec(memory_space=pltpu.VMEM)
    return pl.pallas_call(
        front_kernel,
        out_shape=(
            jax.ShapeDtypeStruct((U, S), F32),
            jax.ShapeDtypeStruct((U, U), F32),
            jax.ShapeDtypeStruct((1, 1, S), F32),
        ),
        in_specs=[vmem_spec] * 5,
        out_specs=(vmem_spec,) * 3,
        scratch_shapes=[
            pltpu.VMEM((2, F, CU), BF16),
            pltpu.VMEM((S, 2 * S), F32),
            pltpu.VMEM((2, CU, CU), BF16),
            pltpu.VMEM((2, CU, CU), BF16),
        ],
        name="front_factor",
    )(child_map, near, following, far, panel)


def scatter_kernel(
    lhat_ref, rest_ref, negative_ref, lhat_out, rest_out, share_out,
    counts, send_sem, recv_sem, count_send, count_recv, row_send, row_recv, own_sem
):
    me = lax.axis_index("row")
    col = lax.axis_index("col")
    others = [peer(me, dx, dz) for dx, dz in OFFSETS]
    columns = [lax.rem(col + d, N_COL) for d in range(1, N_COL)]

    def rows(row):
        return pl.ds(pl.multiple_of(row * UP, SP), UP)

    own = [
        pltpu.make_async_copy(negative_ref, counts.at[me, pl.ds(col, 1)], own_sem.at[0]),
        pltpu.make_async_copy(lhat_ref.at[rows(me)], lhat_out.at[me], own_sem.at[1]),
        pltpu.make_async_copy(rest_ref.at[rows(me)], rest_out.at[me], own_sem.at[2]),
    ]
    for copy in own:
        copy.start()
    greet(others, columns)
    tallies = []
    for place, other in enumerate(columns):
        tallies.append(
            pltpu.make_async_remote_copy(
                src_ref=negative_ref,
                dst_ref=counts.at[me, pl.ds(col, 1)],
                send_sem=count_send.at[place],
                recv_sem=count_recv.at[place],
                device_id={"col": other},
                device_id_type=MESH,
            )
        )
        tallies[-1].start()
    copies = []
    for place, other in enumerate(others):
        for i, (source, target) in enumerate(((lhat_ref, lhat_out), (rest_ref, rest_out))):
            copies.append(
                pltpu.make_async_remote_copy(
                    src_ref=source.at[rows(other)],
                    dst_ref=target.at[me],
                    send_sem=send_sem.at[place, i],
                    recv_sem=recv_sem.at[place, i],
                    device_id={"row": other},
                    device_id_type=MESH,
                )
            )
            copies[-1].start()
    for copy in own:
        copy.wait()
    for copy in tallies:
        copy.wait()
    forwards = []
    for place, other in enumerate(others):
        forwards.append(
            pltpu.make_async_remote_copy(
                src_ref=counts.at[me],
                dst_ref=counts.at[me],
                send_sem=row_send.at[place],
                recv_sem=row_recv.at[place],
                device_id={"row": other},
                device_id_type=MESH,
            )
        )
        forwards[-1].start()
    for copy in copies:
        copy.wait()
    for copy in forwards:
        copy.wait()
    total = counts[0]
    for row in range(1, N_ROW):
        total = total + counts[row]
    flat = jnp.sum(total, axis=0)
    share_out[...] = jnp.sum(flat, axis=1, keepdims=True) / float(N_ROW * N_COL * S)


def scatter(lhat, rest, negative):
    any_spec = pl.BlockSpec(memory_space=pl.ANY)
    vmem_spec = pl.BlockSpec(memory_space=pltpu.VMEM)
    count = len(OFFSETS)
    return pl.pallas_call(
        scatter_kernel,
        out_shape=(
            jax.ShapeDtypeStruct((N_ROW, UP, S), F32),
            jax.ShapeDtypeStruct((N_ROW, UP, U), F32),
            jax.ShapeDtypeStruct((1, 1), F32),
        ),
        in_specs=[any_spec] * 3,
        out_specs=(vmem_spec,) * 3,
        scratch_shapes=[
            pltpu.VMEM((N_ROW, N_COL, 1, S), F32),
            pltpu.SemaphoreType.DMA((count, 2)),
            pltpu.SemaphoreType.DMA((count, 2)),
            pltpu.SemaphoreType.DMA((N_COL - 1,)),
            pltpu.SemaphoreType.DMA((N_COL - 1,)),
            pltpu.SemaphoreType.DMA((count,)),
            pltpu.SemaphoreType.DMA((count,)),
            pltpu.SemaphoreType.DMA((3,)),
        ],
        compiler_params=pltpu.CompilerParams(collective_id=1, has_side_effects=True),
        name="scatter_fronts",
    )(lhat, rest, negative)


def local(front_pivot, front_update, child_blocks, child_map):
    near, following, far, panel = gather(child_blocks, front_pivot, front_update)
    lhat, rest, negative = front(child_map, near, following, far, panel)
    lhat, rest, share = scatter(lhat, rest, negative)
    return (lhat, front_update[:, :, S:] + rest, share[0, 0])


def solution(mesh):
    in_specs = (
        P("col", "row", None),
        P("col", "row", None),
        P("col", None, "row", None),
        P("col", None, None),
    )
    out_specs = (P("col", "row", None), P("col", "row", None), P())
    return jax.shard_map(local, mesh=mesh, in_specs=in_specs, out_specs=out_specs, check_vma=False)
```

```python
import functools

import jax
import jax.numpy as jnp
from jax import lax
from jax.experimental import pallas as pl
from jax.experimental.pallas import tpu as pltpu
from jax.sharding import PartitionSpec as P

MESH = pl.DeviceIdType.MESH
F32 = jnp.float32
BF16 = jnp.bfloat16
HIGHEST = lax.Precision.HIGHEST

N_ROW = 16
N_COL = 8
SIDE = 4
S = 128
CU = 512
U = 640
F = 768
SP = 8
UP = 40
HELD = 32
OFFSETS = [
    (dx, (dx + turn) % SIDE)
    for turn in range(SIDE)
    for dx in range(SIDE)
    if (dx, (dx + turn) % SIDE) != (0, 0)
]


def peer(me, dx, dz):
    x = lax.rem(me // SIDE + dx, SIDE)
    z = lax.rem(lax.rem(me, SIDE) + dz, SIDE)
    return x * SIDE + z


def greet(row_peers, col_peers):
    barrier = pltpu.get_barrier_semaphore()
    for other in row_peers:
        pl.semaphore_signal(barrier, inc=1, device_id={"row": other}, device_id_type=MESH)
    for other in col_peers:
        pl.semaphore_signal(barrier, inc=1, device_id={"col": other}, device_id_type=MESH)
    pl.semaphore_wait(barrier, len(row_peers) + len(col_peers))


def gather_kernel(
    child_ref, pivot_ref, update_ref, near_ref, next_ref, far_ref, panel_ref, send_sem, recv_sem, own_sem
):
    me = lax.axis_index("row")
    group = me // SIDE
    near = pl.multiple_of(group * 128, 128)
    following = pl.multiple_of(lax.rem(group + 1, 4) * 128, 128)
    opposite = pl.multiple_of(lax.rem(group + 2, 4) * 128, 128)
    far_child = group // 2
    rows = pl.ds(pl.multiple_of(me * HELD, HELD), HELD)
    pivot_rows = pl.ds(pl.multiple_of(me * SP, SP), SP)
    update_rows = pl.ds(pl.multiple_of(S + me * UP, SP), UP)

    def pieces(front):
        return (
            (pivot_ref.at[front], panel_ref.at[pivot_rows]),
            (child_ref.at[front, :, :, pl.ds(near, 128)], near_ref.at[:, rows]),
            (child_ref.at[front, :, :, pl.ds(following, 128)], next_ref.at[:, rows]),
            (child_ref.at[front, far_child, :, pl.ds(opposite, 128)], far_ref.at[rows]),
            (update_ref.at[front, :, pl.ds(0, S)], panel_ref.at[update_rows]),
        )

    own = [
        pltpu.make_async_copy(source, target, own_sem.at[i])
        for i, (source, target) in enumerate(pieces(me))
    ]
    for copy in own:
        copy.start()
    others = [peer(me, dx, dz) for dx, dz in OFFSETS]
    greet(others, [])
    copies = []
    for place, other in enumerate(others):
        for i, (source, target) in enumerate(pieces(other)):
            copies.append(
                pltpu.make_async_remote_copy(
                    src_ref=source,
                    dst_ref=target,
                    send_sem=send_sem.at[place, i],
                    recv_sem=recv_sem.at[place, i],
                    device_id={"row": other},
                    device_id_type=MESH,
                )
            )
            copies[-1].start()
    for copy in own:
        copy.wait()
    for copy in copies:
        copy.wait()


def gather(child_blocks, front_pivot, front_update):
    any_spec = pl.BlockSpec(memory_space=pl.ANY)
    vmem_spec = pl.BlockSpec(memory_space=pltpu.VMEM)
    return pl.pallas_call(
        gather_kernel,
        out_shape=(
            jax.ShapeDtypeStruct((2, CU, 128), F32),
            jax.ShapeDtypeStruct((2, CU, 128), F32),
            jax.ShapeDtypeStruct((CU, 128), F32),
            jax.ShapeDtypeStruct((F, S), F32),
        ),
        in_specs=[any_spec] * 3,
        out_specs=(vmem_spec,) * 4,
        scratch_shapes=[
            pltpu.SemaphoreType.DMA((len(OFFSETS), 5)),
            pltpu.SemaphoreType.DMA((len(OFFSETS), 5)),
            pltpu.SemaphoreType.DMA((5,)),
        ],
        compiler_params=pltpu.CompilerParams(collective_id=0, has_side_effects=True),
        name="gather_fronts",
    )(child_blocks, front_pivot, front_update)


def split(values):
    high = values.astype(BF16)
    low = (values - high.astype(F32)).astype(BF16)
    return high, low


def nt_dot(a, b, precision=None):
    return lax.dot_general(
        a, b, (((1,), (1,)), ((), ())), precision=precision, preferred_element_type=F32
    )


BLOCK = 32


def spread_lane(values, lane):
    return jnp.broadcast_to(values[:, lane : lane + 1], (8, 128))


def spread_row(values, row):
    return jnp.broadcast_to(values[row : row + 1, :], (8, 128))


def factor_in_place(work):
    sub = lax.broadcasted_iota(jnp.int32, (8, 128), 0)
    groups = BLOCK // 8
    for block in range(S // BLOCK):
        base = block * BLOCK
        left = [work[base + 8 * g : base + 8 * g + 8, 0:128] for g in range(groups)]
        right = [work[base + 8 * g : base + 8 * g + 8, 128:256] for g in range(groups)]
        for panel in range(groups):
            active = range(panel, groups)
            columns = [
                {g: spread_lane(left[g], base + 8 * panel + j) for g in active} for j in range(8)
            ]
            for j in range(8):
                scale = 1.0 / spread_row(columns[j][panel], j)
                row_left = spread_row(left[panel], j)
                row_right = spread_row(right[panel], j)
                across = {i: spread_row(columns[i][panel], j) for i in range(j + 1, 8)}
                for g in active:
                    multiplier = columns[j][g] * scale
                    if g == panel:
                        multiplier = jnp.where(sub > j, multiplier, 0.0)
                    for i in range(j + 1, 8):
                        columns[i][g] = columns[i][g] - multiplier * across[i]
                    left[g] = left[g] - multiplier * row_left
                    right[g] = right[g] - multiplier * row_right
        strip_left = jnp.concatenate(left, axis=0)
        strip_right = jnp.concatenate(right, axis=0)
        work[base : base + BLOCK, 0:128] = strip_left
        work[base : base + BLOCK, 128:256] = strip_right
        after = base + BLOCK
        if after < S:
            lanes = lax.broadcasted_iota(jnp.int32, (BLOCK, 128), 1)
            places = lax.broadcasted_iota(jnp.int32, (BLOCK, 128), 0) + base
            diagonal = jnp.sum(
                jnp.where(lanes == places, strip_left, 0.0), axis=1, keepdims=True
            )
            lower = strip_left / diagonal
            strip = jnp.concatenate([strip_left, strip_right], axis=1)
            product = lax.dot_general(
                lower, strip, (((0,), (0,)), ((), ())), precision=HIGHEST, preferred_element_type=F32
            )
            work[after:S, :] = work[after:S, :] - product[after:S, :]


def front_kernel(
    map_ref, near_ref, next_ref, far_ref, panel_ref, lhat_ref, rest_ref, negative_ref, hot_ref, work, high_ref, low_ref
):
    me = lax.axis_index("row")
    for child in range(2):
        indices = map_ref[me, child : child + 1, :]
        position = lax.broadcasted_iota(jnp.int32, (F, CU), 0)
        hot_ref[child] = jnp.where(indices == position, 1.0, 0.0).astype(BF16)

    def fill(child, i, j, block):
        high, low = split(block)
        high_ref[child, 128 * i : 128 * i + 128, 128 * j : 128 * j + 128] = high
        low_ref[child, 128 * i : 128 * i + 128, 128 * j : 128 * j + 128] = low

    for child in range(2):
        for i in range(4):
            rows = slice(128 * i, 128 * i + 128)
            fill(child, i, i, near_ref[child, rows, :])
            block = next_ref[child, rows, :]
            fill(child, i, (i + 1) % 4, block)
            fill(child, (i + 1) % 4, i, block.T)
    for i in range(4):
        child = i // 2
        block = far_ref[128 * i : 128 * i + 128, :]
        fill(child, i, (i + 2) % 4, block)
        fill(child, (i + 2) % 4, i, block.T)

    spread = []
    for child in range(2):
        hot = hot_ref[child]
        high = jnp.dot(hot, high_ref[child], preferred_element_type=F32).astype(BF16)
        low = jnp.dot(hot, low_ref[child], preferred_element_type=F32).astype(BF16)
        spread.append((high, low))

    def columns(start, size, first=0):
        total = None
        for child in range(2):
            hot = hot_ref[child, start : start + size, :]
            for part in spread[child]:
                term = nt_dot(part[first:, :], hot)
                total = term if total is None else total + term
        return total

    panel = panel_ref[...] + columns(0, S)
    lane = lax.broadcasted_iota(jnp.int32, (S, S), 1)
    place = lax.broadcasted_iota(jnp.int32, (S, S), 0)
    work[:, 0:128] = panel[:S]
    work[:, 128:256] = jnp.where(lane == place, 1.0, 0.0)
    factor_in_place(work)
    inverse = work[:, 128:256]
    pivots = jnp.sum(jnp.where(lane == place, work[:, 0:128], 0.0), axis=0, keepdims=True)
    negative_ref[0] = jnp.where(pivots < 0.0, 1.0, 0.0)
    lhat = nt_dot(panel[S:], inverse, HIGHEST)
    lhat_ref[...] = lhat
    scaled = lhat / pivots
    for start in range(0, U, 128):
        correction = nt_dot(scaled, lhat[start : start + 128], HIGHEST)
        rest_ref[:, start : start + 128] = columns(S + start, 128, S) - correction


def front(child_map, near, following, far, panel):
    vmem_spec = pl.BlockSpec(memory_space=pltpu.VMEM)
    return pl.pallas_call(
        front_kernel,
        out_shape=(
            jax.ShapeDtypeStruct((U, S), F32),
            jax.ShapeDtypeStruct((U, U), F32),
            jax.ShapeDtypeStruct((1, 1, S), F32),
        ),
        in_specs=[vmem_spec] * 5,
        out_specs=(vmem_spec,) * 3,
        scratch_shapes=[
            pltpu.VMEM((2, F, CU), BF16),
            pltpu.VMEM((S, 2 * S), F32),
            pltpu.VMEM((2, CU, CU), BF16),
            pltpu.VMEM((2, CU, CU), BF16),
        ],
        name="front_factor",
    )(child_map, near, following, far, panel)


def scatter_kernel(
    lhat_ref, rest_ref, negative_ref, lhat_out, rest_out, share_out,
    counts, send_sem, recv_sem, count_send, count_recv, row_send, row_recv, own_sem
):
    me = lax.axis_index("row")
    col = lax.axis_index("col")
    others = [peer(me, dx, dz) for dx, dz in OFFSETS]
    columns = [lax.rem(col + d, N_COL) for d in range(1, N_COL)]

    def rows(row):
        return pl.ds(pl.multiple_of(row * UP, SP), UP)

    own = [
        pltpu.make_async_copy(negative_ref, counts.at[me, pl.ds(col, 1)], own_sem.at[0]),
        pltpu.make_async_copy(lhat_ref.at[rows(me)], lhat_out.at[me], own_sem.at[1]),
        pltpu.make_async_copy(rest_ref.at[rows(me)], rest_out.at[me], own_sem.at[2]),
    ]
    for copy in own:
        copy.start()
    greet(others, columns)
    tallies = []
    for place, other in enumerate(columns):
        tallies.append(
            pltpu.make_async_remote_copy(
                src_ref=negative_ref,
                dst_ref=counts.at[me, pl.ds(col, 1)],
                send_sem=count_send.at[place],
                recv_sem=count_recv.at[place],
                device_id={"col": other},
                device_id_type=MESH,
            )
        )
        tallies[-1].start()
    copies = []
    for place, other in enumerate(others):
        for i, (source, target) in enumerate(((lhat_ref, lhat_out), (rest_ref, rest_out))):
            copies.append(
                pltpu.make_async_remote_copy(
                    src_ref=source.at[rows(other)],
                    dst_ref=target.at[me],
                    send_sem=send_sem.at[place, i],
                    recv_sem=recv_sem.at[place, i],
                    device_id={"row": other},
                    device_id_type=MESH,
                )
            )
            copies[-1].start()
    for copy in own:
        copy.wait()
    for copy in tallies:
        copy.wait()
    forwards = []
    for place, other in enumerate(others):
        forwards.append(
            pltpu.make_async_remote_copy(
                src_ref=counts.at[me],
                dst_ref=counts.at[me],
                send_sem=row_send.at[place],
                recv_sem=row_recv.at[place],
                device_id={"row": other},
                device_id_type=MESH,
            )
        )
        forwards[-1].start()
    for copy in copies:
        copy.wait()
    for copy in forwards:
        copy.wait()
    total = counts[0]
    for row in range(1, N_ROW):
        total = total + counts[row]
    flat = jnp.sum(total, axis=0)
    share_out[...] = jnp.sum(flat, axis=1, keepdims=True) / float(N_ROW * N_COL * S)


def scatter(lhat, rest, negative):
    any_spec = pl.BlockSpec(memory_space=pl.ANY)
    vmem_spec = pl.BlockSpec(memory_space=pltpu.VMEM)
    count = len(OFFSETS)
    return pl.pallas_call(
        scatter_kernel,
        out_shape=(
            jax.ShapeDtypeStruct((N_ROW, UP, S), F32),
            jax.ShapeDtypeStruct((N_ROW, UP, U), F32),
            jax.ShapeDtypeStruct((1, 1), F32),
        ),
        in_specs=[any_spec] * 3,
        out_specs=(vmem_spec,) * 3,
        scratch_shapes=[
            pltpu.VMEM((N_ROW, N_COL, 1, S), F32),
            pltpu.SemaphoreType.DMA((count, 2)),
            pltpu.SemaphoreType.DMA((count, 2)),
            pltpu.SemaphoreType.DMA((N_COL - 1,)),
            pltpu.SemaphoreType.DMA((N_COL - 1,)),
            pltpu.SemaphoreType.DMA((count,)),
            pltpu.SemaphoreType.DMA((count,)),
            pltpu.SemaphoreType.DMA((3,)),
        ],
        compiler_params=pltpu.CompilerParams(collective_id=1, has_side_effects=True),
        name="scatter_fronts",
    )(lhat, rest, negative)


def local(front_pivot, front_update, child_blocks, child_map):
    near, following, far, panel = gather(child_blocks, front_pivot, front_update)
    lhat, rest, negative = front(child_map, near, following, far, panel)
    lhat, rest, share = scatter(lhat, rest, negative)
    return (lhat, front_update[:, :, S:] + rest, share[0, 0])


def solution(mesh):
    in_specs = (
        P("col", "row", None),
        P("col", "row", None),
        P("col", None, "row", None),
        P("col", None, None),
    )
    out_specs = (P("col", "row", None), P("col", "row", None), P())
    return jax.shard_map(local, mesh=mesh, in_specs=in_specs, out_specs=out_specs, check_vma=False)
```

```python
import jax
import jax.numpy as jnp
from jax import lax
from jax.experimental import pallas as pl
from jax.experimental.pallas import tpu as pltpu
from jax.sharding import PartitionSpec as P

MESH = pl.DeviceIdType.MESH
F32 = jnp.float32
BF16 = jnp.bfloat16
HIGHEST = lax.Precision.HIGHEST

N_ROW = 16
N_COL = 8
SIDE = 4
S = 128
CU = 512
U = 640
F = 768
SP = 8
UP = 40
HELD = 32
BLOCK = 32
OFFSETS = [
    (dx, (dx + turn) % SIDE)
    for turn in range(SIDE)
    for dx in range(SIDE)
    if (dx, (dx + turn) % SIDE) != (0, 0)
]
PEERS = len(OFFSETS)
PIECES = 7


def peer(me, dx, dz):
    x = lax.rem(me // SIDE + dx, SIDE)
    z = lax.rem(lax.rem(me, SIDE) + dz, SIDE)
    return x * SIDE + z


def to_row(source, target, send_sem, recv_sem, row):
    return pltpu.make_async_remote_copy(
        src_ref=source,
        dst_ref=target,
        send_sem=send_sem,
        recv_sem=recv_sem,
        device_id={"row": row},
        device_id_type=MESH,
    )


def split(values):
    high = values.astype(BF16)
    low = (values - high.astype(F32)).astype(BF16)
    return high, low


def nt_dot(a, b, precision=None):
    return lax.dot_general(
        a, b, (((1,), (1,)), ((), ())), precision=precision, preferred_element_type=F32
    )


def spread_lane(values, lane):
    return jnp.broadcast_to(values[:, lane : lane + 1], (8, 128))


def spread_row(values, row):
    return jnp.broadcast_to(values[row : row + 1, :], (8, 128))


def factor_in_place(work, meanwhile):
    sub = lax.broadcasted_iota(jnp.int32, (8, 128), 0)
    groups = BLOCK // 8
    for block in range(S // BLOCK):
        base = block * BLOCK
        left = [work[base + 8 * g : base + 8 * g + 8, 0:128] for g in range(groups)]
        right = [work[base + 8 * g : base + 8 * g + 8, 128:256] for g in range(groups)]
        for panel in range(groups):
            active = range(panel, groups)
            columns = [
                {g: spread_lane(left[g], base + 8 * panel + j) for g in active} for j in range(8)
            ]
            for j in range(8):
                scale = 1.0 / spread_row(columns[j][panel], j)
                row_left = spread_row(left[panel], j)
                row_right = spread_row(right[panel], j)
                across = {i: spread_row(columns[i][panel], j) for i in range(j + 1, 8)}
                for g in active:
                    multiplier = columns[j][g] * scale
                    if g == panel:
                        multiplier = jnp.where(sub > j, multiplier, 0.0)
                    for i in range(j + 1, 8):
                        columns[i][g] = columns[i][g] - multiplier * across[i]
                    left[g] = left[g] - multiplier * row_left
                    right[g] = right[g] - multiplier * row_right
            if meanwhile:
                meanwhile.pop(0)()
        strip_left = jnp.concatenate(left, axis=0)
        strip_right = jnp.concatenate(right, axis=0)
        work[base : base + BLOCK, 0:128] = strip_left
        work[base : base + BLOCK, 128:256] = strip_right
        after = base + BLOCK
        if after < S:
            lanes = lax.broadcasted_iota(jnp.int32, (BLOCK, 128), 1)
            places = lax.broadcasted_iota(jnp.int32, (BLOCK, 128), 0) + base
            diagonal = jnp.sum(
                jnp.where(lanes == places, strip_left, 0.0), axis=1, keepdims=True
            )
            lower = strip_left / diagonal
            strip = jnp.concatenate([strip_left, strip_right], axis=1)
            product = lax.dot_general(
                lower, strip, (((0,), (0,)), ((), ())), precision=HIGHEST, preferred_element_type=F32
            )
            work[after:S, :] = work[after:S, :] - product[after:S, :]
    while meanwhile:
        meanwhile.pop(0)()


def fronts_kernel(
    child_ref, pivot_ref, update_ref, map_ref, lhat_out, rest_out, share_out,
    maps, near_ref, next_ref, far_ref, panel_ref, hot_ref, high_ref, low_ref, spread_ref, work,
    lhat_ref, rest_ref, negative_ref, counts,
    own_sem, in_send, in_recv, out_send, out_recv, count_send, count_recv, row_send, row_recv,
):
    me = lax.axis_index("row")
    col = lax.axis_index("col")
    others = [peer(me, dx, dz) for dx, dz in OFFSETS]
    columns = [lax.rem(col + d, N_COL) for d in range(1, N_COL)]

    barrier = pltpu.get_barrier_semaphore()
    for other in others:
        pl.semaphore_signal(barrier, inc=1, device_id={"row": other}, device_id_type=MESH)
    for other in columns:
        pl.semaphore_signal(barrier, inc=1, device_id={"col": other}, device_id_type=MESH)

    group = me // SIDE
    near = pl.multiple_of(group * 128, 128)
    following = pl.multiple_of(lax.rem(group + 1, 4) * 128, 128)
    opposite = pl.multiple_of(lax.rem(group + 2, 4) * 128, 128)
    far_child = group // 2
    held = pl.ds(pl.multiple_of(me * HELD, HELD), HELD)
    pivot_rows = pl.ds(pl.multiple_of(me * SP, SP), SP)
    update_rows = pl.ds(pl.multiple_of(S + me * UP, SP), UP)

    def pieces(front):
        return (
            (pivot_ref.at[front], panel_ref.at[pivot_rows]),
            (child_ref.at[front, 0, :, pl.ds(near, 128)], near_ref.at[0, held]),
            (child_ref.at[front, 0, :, pl.ds(following, 128)], next_ref.at[0, held]),
            (child_ref.at[front, far_child, :, pl.ds(opposite, 128)], far_ref.at[held]),
            (child_ref.at[front, 1, :, pl.ds(near, 128)], near_ref.at[1, held]),
            (child_ref.at[front, 1, :, pl.ds(following, 128)], next_ref.at[1, held]),
            (update_ref.at[front, :, pl.ds(0, S)], panel_ref.at[update_rows]),
        )

    map_copy = pltpu.make_async_copy(map_ref.at[me], maps, own_sem.at[PIECES])
    map_copy.start()
    own = [
        pltpu.make_async_copy(source, target, own_sem.at[i])
        for i, (source, target) in enumerate(pieces(me))
    ]
    for copy in own:
        copy.start()
    pl.semaphore_wait(barrier, PEERS + N_COL - 1)
    incoming = [
        [
            to_row(*pieces(other)[i], in_send.at[place, i], in_recv.at[place, i], other)
            for place, other in enumerate(others)
        ]
        for i in range(PIECES)
    ]
    for kind in incoming:
        for copy in kind:
            copy.start()

    def arrived(kinds):
        for i in kinds:
            own[i].wait()
            for copy in incoming[i]:
                copy.wait_recv()

    map_copy.wait()
    for child in range(2):
        indices = maps[child : child + 1, :]
        position = lax.broadcasted_iota(jnp.int32, (F, CU), 0)
        hot_ref[child] = jnp.where(indices == position, 1.0, 0.0).astype(BF16)

    def fill(i, j, block):
        high, low = split(block)
        high_ref[128 * i : 128 * i + 128, 128 * j : 128 * j + 128] = high
        low_ref[128 * i : 128 * i + 128, 128 * j : 128 * j + 128] = low

    def spread_child(child):
        for i in range(4):
            rows = slice(128 * i, 128 * i + 128)
            fill(i, i, near_ref[child, rows, :])
            block = next_ref[child, rows, :]
            fill(i, (i + 1) % 4, block)
            fill((i + 1) % 4, i, block.T)
        for i in (2 * child, 2 * child + 1):
            block = far_ref[128 * i : 128 * i + 128, :]
            fill(i, (i + 2) % 4, block)
            fill((i + 2) % 4, i, block.T)
        for part, ref in enumerate((high_ref, low_ref)):
            spread_ref[child, part] = jnp.dot(
                hot_ref[child], ref[...], preferred_element_type=F32
            ).astype(BF16)

    def placed(start, size, first, count):
        total = None
        for child in range(2):
            hot = hot_ref[child, start : start + size, :]
            for part in range(2):
                term = nt_dot(spread_ref[child, part, first : first + count, :], hot)
                total = term if total is None else total + term
        return total

    arrived((0, 1, 2, 3))
    spread_child(0)
    arrived((4, 5))
    spread_child(1)
    early = placed(0, 256, 0, F)
    rest_ref[:, 0:128] = early[S:, 128:256]
    lane = lax.broadcasted_iota(jnp.int32, (S, S), 1)
    place = lax.broadcasted_iota(jnp.int32, (S, S), 0)
    work[:, 0:128] = panel_ref[0:S, :] + early[0:S, 0:128]
    work[:, 128:256] = jnp.where(lane == place, 1.0, 0.0)

    def later(start, first):
        def run():
            rest_ref[first : first + 160, start : start + 256] = placed(S + start, 256, S + first, 160)
        return run

    factor_in_place(work, [later(start, first) for start in (128, 384) for first in range(0, U, 160)])
    inverse = work[:, 128:256]
    pivots = jnp.sum(jnp.where(lane == place, work[:, 0:128], 0.0), axis=0, keepdims=True)
    negative = jnp.where(pivots < 0.0, 1.0, 0.0)
    negative_ref[0] = negative
    counts[me, pl.ds(col, 1)] = negative[None]
    tallies = []
    for i, other in enumerate(columns):
        tallies.append(
            pltpu.make_async_remote_copy(
                src_ref=negative_ref,
                dst_ref=counts.at[me, pl.ds(col, 1)],
                send_sem=count_send.at[i],
                recv_sem=count_recv.at[i],
                device_id={"col": other},
                device_id_type=MESH,
            )
        )
        tallies[-1].start()
    arrived((6,))
    lhat = nt_dot(panel_ref[S:, :] + early[S:, 0:128], inverse, HIGHEST)
    lhat_ref[...] = lhat

    def share(row):
        return pl.ds(pl.multiple_of(row * UP, SP), UP)

    outgoing = [
        [
            to_row(
                source.at[share(other)], target.at[me], out_send.at[i, kind], out_recv.at[i, kind], other
            )
            for i, other in enumerate(others)
        ]
        for kind, (source, target) in enumerate(((lhat_ref, lhat_out), (rest_ref, rest_out)))
    ]
    for copy in outgoing[0]:
        copy.start()
    scaled = lhat / pivots
    for start, size in ((0, 256), (256, 256), (512, 128)):
        correction = nt_dot(scaled, lhat[start : start + size], HIGHEST)
        rest_ref[:, start : start + size] = rest_ref[:, start : start + size] - correction
    for copy in tallies:
        copy.wait()
    forwards = [
        to_row(counts.at[me], counts.at[me], row_send.at[i], row_recv.at[i], other)
        for i, other in enumerate(others)
    ]
    for copy in forwards:
        copy.start()
    for copy in outgoing[1]:
        copy.start()
    lhat_out[me] = lhat_ref[share(me), :]
    rest_out[me] = rest_ref[share(me), :]
    for copy in forwards:
        copy.wait()
    total = counts[0]
    for row in range(1, N_ROW):
        total = total + counts[row]
    flat = jnp.sum(total, axis=0)
    share_out[...] = jnp.sum(flat, axis=1, keepdims=True) / float(N_ROW * N_COL * S)
    for kind in outgoing:
        for copy in kind:
            copy.wait()
    for kind in incoming:
        for copy in kind:
            copy.wait_send()


def fronts(child_blocks, front_pivot, front_update, child_map):
    any_spec = pl.BlockSpec(memory_space=pl.ANY)
    vmem_spec = pl.BlockSpec(memory_space=pltpu.VMEM)
    dma = pltpu.SemaphoreType.DMA
    return pl.pallas_call(
        fronts_kernel,
        out_shape=(
            jax.ShapeDtypeStruct((N_ROW, UP, S), F32),
            jax.ShapeDtypeStruct((N_ROW, UP, U), F32),
            jax.ShapeDtypeStruct((1, 1), F32),
        ),
        in_specs=[any_spec] * 4,
        out_specs=(vmem_spec,) * 3,
        scratch_shapes=[
            pltpu.VMEM((2, CU), jnp.int32),
            pltpu.VMEM((2, CU, 128), F32),
            pltpu.VMEM((2, CU, 128), F32),
            pltpu.VMEM((CU, 128), F32),
            pltpu.VMEM((F, S), F32),
            pltpu.VMEM((2, F, CU), BF16),
            pltpu.VMEM((CU, CU), BF16),
            pltpu.VMEM((CU, CU), BF16),
            pltpu.VMEM((2, 2, F, CU), BF16),
            pltpu.VMEM((S, 2 * S), F32),
            pltpu.VMEM((U, S), F32),
            pltpu.VMEM((U, U), F32),
            pltpu.VMEM((1, 1, S), F32),
            pltpu.VMEM((N_ROW, N_COL, 1, S), F32),
            dma((PIECES + 1,)),
            dma((PEERS, PIECES)),
            dma((PEERS, PIECES)),
            dma((PEERS, 2)),
            dma((PEERS, 2)),
            dma((N_COL - 1,)),
            dma((N_COL - 1,)),
            dma((PEERS,)),
            dma((PEERS,)),
        ],
        compiler_params=pltpu.CompilerParams(collective_id=0, has_side_effects=True),
        name="fronts",
    )(child_blocks, front_pivot, front_update, child_map)


def local(front_pivot, front_update, child_blocks, child_map):
    lhat, rest, share = fronts(child_blocks, front_pivot, front_update, child_map)
    return (lhat, front_update[:, :, S:] + rest, share[0, 0])


def solution(mesh):
    in_specs = (
        P("col", "row", None),
        P("col", "row", None),
        P("col", None, "row", None),
        P("col", None, None),
    )
    out_specs = (P("col", "row", None), P("col", "row", None), P())
    return jax.shard_map(local, mesh=mesh, in_specs=in_specs, out_specs=out_specs, check_vma=False)
```

```python
import jax
import jax.numpy as jnp
from jax import lax
from jax.experimental import pallas as pl
from jax.experimental.pallas import tpu as pltpu
from jax.sharding import PartitionSpec as P

MESH = pl.DeviceIdType.MESH
F32 = jnp.float32
BF16 = jnp.bfloat16
HIGHEST = lax.Precision.HIGHEST

N_ROW = 16
N_COL = 8
SIDE = 4
S = 128
CU = 512
U = 640
F = 768
SP = 8
UP = 40
HELD = 32
BLOCK = 32
OFFSETS = [
    (dx, (dx + turn) % SIDE)
    for turn in range(SIDE)
    for dx in range(SIDE)
    if (dx, (dx + turn) % SIDE) != (0, 0)
]
PEERS = len(OFFSETS)
PIECES = 7


def peer(me, dx, dz):
    x = lax.rem(me // SIDE + dx, SIDE)
    z = lax.rem(lax.rem(me, SIDE) + dz, SIDE)
    return x * SIDE + z


def to_row(source, target, send_sem, recv_sem, row):
    return pltpu.make_async_remote_copy(
        src_ref=source,
        dst_ref=target,
        send_sem=send_sem,
        recv_sem=recv_sem,
        device_id={"row": row},
        device_id_type=MESH,
    )


def split(values):
    high = values.astype(BF16)
    low = (values - high.astype(F32)).astype(BF16)
    return high, low


def nt_dot(a, b, precision=None):
    return lax.dot_general(
        a, b, (((1,), (1,)), ((), ())), precision=precision, preferred_element_type=F32
    )


def spread_lane(values, lane):
    return jnp.broadcast_to(values[:, lane : lane + 1], (8, 128))


def spread_row(values, row):
    return jnp.broadcast_to(values[row : row + 1, :], (8, 128))


def factor_in_place(work, meanwhile):
    sub = lax.broadcasted_iota(jnp.int32, (8, 128), 0)
    groups = BLOCK // 8
    for block in range(S // BLOCK):
        base = block * BLOCK
        left = [work[base + 8 * g : base + 8 * g + 8, 0:128] for g in range(groups)]
        right = [work[base + 8 * g : base + 8 * g + 8, 128:256] for g in range(groups)]
        for panel in range(groups):
            active = range(panel, groups)
            columns = [
                {g: spread_lane(left[g], base + 8 * panel + j) for g in active} for j in range(8)
            ]
            for j in range(8):
                scale = 1.0 / spread_row(columns[j][panel], j)
                row_left = spread_row(left[panel], j)
                row_right = spread_row(right[panel], j)
                across = {i: spread_row(columns[i][panel], j) for i in range(j + 1, 8)}
                for g in active:
                    multiplier = columns[j][g] * scale
                    if g == panel:
                        multiplier = jnp.where(sub > j, multiplier, 0.0)
                    for i in range(j + 1, 8):
                        columns[i][g] = columns[i][g] - multiplier * across[i]
                    left[g] = left[g] - multiplier * row_left
                    right[g] = right[g] - multiplier * row_right
            if meanwhile and panel % 2 == 0:
                meanwhile.pop(0)()
        strip_left = jnp.concatenate(left, axis=0)
        strip_right = jnp.concatenate(right, axis=0)
        work[base : base + BLOCK, 0:128] = strip_left
        work[base : base + BLOCK, 128:256] = strip_right
        after = base + BLOCK
        if after < S:
            lanes = lax.broadcasted_iota(jnp.int32, (BLOCK, 128), 1)
            places = lax.broadcasted_iota(jnp.int32, (BLOCK, 128), 0) + base
            diagonal = jnp.sum(
                jnp.where(lanes == places, strip_left, 0.0), axis=1, keepdims=True
            )
            lower = strip_left / diagonal
            strip = jnp.concatenate([strip_left, strip_right], axis=1)
            product = lax.dot_general(
                lower, strip, (((0,), (0,)), ((), ())), precision=HIGHEST, preferred_element_type=F32
            )
            work[after:S, :] = work[after:S, :] - product[after:S, :]
    while meanwhile:
        meanwhile.pop(0)()


def fronts_kernel(
    child_ref, pivot_ref, update_ref, map_ref, lhat_out, schur_out, share_out,
    maps, near_ref, next_ref, far_ref, panel_ref, hot_ref, high_ref, low_ref, spread_ref, work,
    lhat_ref, rest_ref, added_ref, landed, trailing, negative_ref, counts,
    own_sem, written_sem, in_send, in_recv, out_send, out_recv, count_send, count_recv, row_send, row_recv,
):
    me = lax.axis_index("row")
    col = lax.axis_index("col")
    others = [peer(me, dx, dz) for dx, dz in OFFSETS]
    columns = [lax.rem(col + d, N_COL) for d in range(1, N_COL)]

    barrier = pltpu.get_barrier_semaphore()
    for other in others:
        pl.semaphore_signal(barrier, inc=1, device_id={"row": other}, device_id_type=MESH)
    for other in columns:
        pl.semaphore_signal(barrier, inc=1, device_id={"col": other}, device_id_type=MESH)

    group = me // SIDE
    near = pl.multiple_of(group * 128, 128)
    following = pl.multiple_of(lax.rem(group + 1, 4) * 128, 128)
    opposite = pl.multiple_of(lax.rem(group + 2, 4) * 128, 128)
    far_child = group // 2
    held = pl.ds(pl.multiple_of(me * HELD, HELD), HELD)
    pivot_rows = pl.ds(pl.multiple_of(me * SP, SP), SP)
    update_rows = pl.ds(pl.multiple_of(S + me * UP, SP), UP)

    def pieces(front):
        return (
            (pivot_ref.at[front], panel_ref.at[pivot_rows]),
            (child_ref.at[front, 0, :, pl.ds(near, 128)], near_ref.at[0, held]),
            (child_ref.at[front, 0, :, pl.ds(following, 128)], next_ref.at[0, held]),
            (child_ref.at[front, far_child, :, pl.ds(opposite, 128)], far_ref.at[held]),
            (child_ref.at[front, 1, :, pl.ds(near, 128)], near_ref.at[1, held]),
            (child_ref.at[front, 1, :, pl.ds(following, 128)], next_ref.at[1, held]),
            (update_ref.at[front, :, pl.ds(0, S)], panel_ref.at[update_rows]),
        )

    map_copy = pltpu.make_async_copy(map_ref.at[me], maps, own_sem.at[PIECES])
    map_copy.start()
    own = [
        pltpu.make_async_copy(source, target, own_sem.at[i])
        for i, (source, target) in enumerate(pieces(me))
    ]
    for copy in own:
        copy.start()
    pl.semaphore_wait(barrier, PEERS + N_COL - 1)
    incoming = [
        [
            to_row(*pieces(other)[i], in_send.at[place, i], in_recv.at[place, i], other)
            for place, other in enumerate(others)
        ]
        for i in range(PIECES)
    ]
    for kind in incoming:
        for copy in kind:
            copy.start()

    def arrived(kinds):
        for i in kinds:
            own[i].wait()
            for copy in incoming[i]:
                copy.wait_recv()

    trailing_copy = pltpu.make_async_copy(
        update_ref.at[:, :, pl.ds(S, U)], trailing, own_sem.at[PIECES + 2]
    )
    trailing_copy.start()
    map_copy.wait()
    for child in range(2):
        indices = maps[child : child + 1, :]
        position = lax.broadcasted_iota(jnp.int32, (F, CU), 0)
        hot_ref[child] = jnp.where(indices == position, 1.0, 0.0).astype(BF16)

    def fill(i, j, block):
        high, low = split(block)
        high_ref[128 * i : 128 * i + 128, 128 * j : 128 * j + 128] = high
        low_ref[128 * i : 128 * i + 128, 128 * j : 128 * j + 128] = low

    def fill_child(child):
        for i in range(4):
            rows = slice(128 * i, 128 * i + 128)
            fill(i, i, near_ref[child, rows, :])
            block = next_ref[child, rows, :]
            fill(i, (i + 1) % 4, block)
            fill((i + 1) % 4, i, block.T)
        for i in (2 * child, 2 * child + 1):
            block = far_ref[128 * i : 128 * i + 128, :]
            fill(i, (i + 2) % 4, block)
            fill((i + 2) % 4, i, block.T)

    def spread_rows(child, first, count):
        for part, ref in enumerate((high_ref, low_ref)):
            spread_ref[child, part, first : first + count, :] = jnp.dot(
                hot_ref[child, first : first + count, :], ref[...], preferred_element_type=F32
            ).astype(BF16)

    def placed(start, size, first, count):
        total = None
        for child in range(2):
            hot = hot_ref[child, start : start + size, :]
            for part in range(2):
                term = nt_dot(spread_ref[child, part, first : first + count, :], hot)
                total = term if total is None else total + term
        return total

    arrived((0, 1, 2, 3))
    fill_child(0)
    spread_rows(0, 0, F)
    arrived((4, 5))
    fill_child(1)
    spread_rows(1, 0, S)
    lane = lax.broadcasted_iota(jnp.int32, (S, S), 1)
    place = lax.broadcasted_iota(jnp.int32, (S, S), 0)
    work[:, 0:128] = panel_ref[0:S, :] + placed(0, S, 0, S)
    work[:, 128:256] = jnp.where(lane == place, 1.0, 0.0)

    def spread_later(first):
        return lambda: spread_rows(1, first, 320)

    def placed_later(start, first):
        def run():
            block = placed(start, 256, first, 320)
            rows = slice(first - S, first - S + 320)
            if start == 0:
                added_ref[rows, :] = block[:, 0:128]
                rest_ref[rows, 0:128] = block[:, 128:256]
            else:
                rest_ref[rows, start - S : start - S + 256] = block
        return run

    halves = (S, S + 320)
    factor_in_place(
        work,
        [spread_later(first) for first in halves]
        + [placed_later(start, first) for start in (0, 256, 512) for first in halves],
    )
    inverse = work[:, 128:256]
    pivots = jnp.sum(jnp.where(lane == place, work[:, 0:128], 0.0), axis=0, keepdims=True)
    negative = jnp.where(pivots < 0.0, 1.0, 0.0)
    negative_ref[0] = negative
    counts[me, pl.ds(col, 1)] = negative[None]
    tallies = []
    for i, other in enumerate(columns):
        tallies.append(
            pltpu.make_async_remote_copy(
                src_ref=negative_ref,
                dst_ref=counts.at[me, pl.ds(col, 1)],
                send_sem=count_send.at[i],
                recv_sem=count_recv.at[i],
                device_id={"col": other},
                device_id_type=MESH,
            )
        )
        tallies[-1].start()
    arrived((6,))
    lhat = nt_dot(panel_ref[S:, :] + added_ref[...], inverse, HIGHEST)
    lhat_ref[...] = lhat

    def share(row):
        return pl.ds(pl.multiple_of(row * UP, SP), UP)

    outgoing = [
        [
            to_row(
                source.at[share(other)], target.at[me], out_send.at[i, kind], out_recv.at[i, kind], other
            )
            for i, other in enumerate(others)
        ]
        for kind, (source, target) in enumerate(((lhat_ref, lhat_out), (rest_ref, landed)))
    ]
    for copy in outgoing[0]:
        copy.start()
    scaled = lhat / pivots
    for start, size in ((0, 256), (256, 256), (512, 128)):
        correction = nt_dot(scaled, lhat[start : start + size], HIGHEST)
        rest_ref[:, start : start + size] = rest_ref[:, start : start + size] - correction
    for copy in outgoing[1]:
        copy.start()
    own_lhat = pltpu.make_async_copy(lhat_ref.at[share(me)], lhat_out.at[me], own_sem.at[PIECES + 1])
    own_lhat.start()
    for copy in tallies:
        copy.wait()
    forwards = [
        to_row(counts.at[me], counts.at[me], row_send.at[i], row_recv.at[i], other)
        for i, other in enumerate(others)
    ]
    for copy in forwards:
        copy.start()
    trailing_copy.wait()
    written = [pltpu.make_async_copy(trailing.at[me], schur_out.at[me], written_sem.at[PEERS])]
    trailing[me] = trailing[me] + rest_ref[share(me), :]
    written[0].start()
    for i, (dx, dz) in enumerate(OFFSETS):
        outgoing[1][i].wait_recv()
        source = peer(me, (SIDE - dx) % SIDE, (SIDE - dz) % SIDE)
        trailing[source] = trailing[source] + landed[source]
        copy = pltpu.make_async_copy(trailing.at[source], schur_out.at[source], written_sem.at[i])
        copy.start()
        written.append(copy)
    for copy in forwards:
        copy.wait()
    total = counts[0]
    for row in range(1, N_ROW):
        total = total + counts[row]
    flat = jnp.sum(total, axis=0)
    share_out[...] = jnp.sum(flat, axis=1, keepdims=True) / float(N_ROW * N_COL * S)
    for copy in outgoing[0]:
        copy.wait()
    for copy in outgoing[1]:
        copy.wait_send()
    for kind in incoming:
        for copy in kind:
            copy.wait_send()
    own_lhat.wait()
    for copy in written:
        copy.wait()


def fronts(child_blocks, front_pivot, front_update, child_map):
    any_spec = pl.BlockSpec(memory_space=pl.ANY)
    vmem_spec = pl.BlockSpec(memory_space=pltpu.VMEM)
    dma = pltpu.SemaphoreType.DMA
    return pl.pallas_call(
        fronts_kernel,
        out_shape=(
            jax.ShapeDtypeStruct((N_ROW, UP, S), F32),
            jax.ShapeDtypeStruct((N_ROW, UP, U), F32),
            jax.ShapeDtypeStruct((1, 1), F32),
        ),
        in_specs=[any_spec] * 4,
        out_specs=(any_spec, any_spec, vmem_spec),
        scratch_shapes=[
            pltpu.VMEM((2, CU), jnp.int32),
            pltpu.VMEM((2, CU, 128), F32),
            pltpu.VMEM((2, CU, 128), F32),
            pltpu.VMEM((CU, 128), F32),
            pltpu.VMEM((F, S), F32),
            pltpu.VMEM((2, F, CU), BF16),
            pltpu.VMEM((CU, CU), BF16),
            pltpu.VMEM((CU, CU), BF16),
            pltpu.VMEM((2, 2, F, CU), BF16),
            pltpu.VMEM((S, 2 * S), F32),
            pltpu.VMEM((U, S), F32),
            pltpu.VMEM((U, U), F32),
            pltpu.VMEM((U, S), F32),
            pltpu.VMEM((N_ROW, UP, U), F32),
            pltpu.VMEM((N_ROW, UP, U), F32),
            pltpu.VMEM((1, 1, S), F32),
            pltpu.VMEM((N_ROW, N_COL, 1, S), F32),
            dma((PIECES + 3,)),
            dma((PEERS + 1,)),
            dma((PEERS, PIECES)),
            dma((PEERS, PIECES)),
            dma((PEERS, 2)),
            dma((PEERS, 2)),
            dma((N_COL - 1,)),
            dma((N_COL - 1,)),
            dma((PEERS,)),
            dma((PEERS,)),
        ],
        compiler_params=pltpu.CompilerParams(collective_id=0, has_side_effects=True),
        name="fronts",
    )(child_blocks, front_pivot, front_update, child_map)


def local(front_pivot, front_update, child_blocks, child_map):
    lhat, schur, share = fronts(child_blocks, front_pivot, front_update, child_map)
    return (lhat, schur, share[0, 0])


def solution(mesh):
    in_specs = (
        P("col", "row", None),
        P("col", "row", None),
        P("col", None, "row", None),
        P("col", None, None),
    )
    out_specs = (P("col", "row", None), P("col", "row", None), P())
    return jax.shard_map(local, mesh=mesh, in_specs=in_specs, out_specs=out_specs, check_vma=False)
```

```python
import jax
import jax.numpy as jnp
from jax import lax
from jax.experimental import pallas as pl
from jax.experimental.pallas import tpu as pltpu
from jax.sharding import PartitionSpec as P

MESH = pl.DeviceIdType.MESH
F32 = jnp.float32
BF16 = jnp.bfloat16
HIGHEST = lax.Precision.HIGHEST

N_ROW = 16
N_COL = 8
SIDE = 4
S = 128
CU = 512
U = 640
F = 768
SP = 8
UP = 40
HELD = 32
BLOCK = 64
OFFSETS = sorted(
    [
        (dx, (turn - dx) % SIDE)
        for turn in range(SIDE)
        for dx in range(SIDE)
        if (dx, (turn - dx) % SIDE) != (0, 0)
    ],
    key=lambda offset: -sum(min(d, SIDE - d) for d in offset),
)
PEERS = len(OFFSETS)
PIECES = 7


def peer(me, dx, dz):
    x = lax.rem(me // SIDE + dx, SIDE)
    z = lax.rem(lax.rem(me, SIDE) + dz, SIDE)
    return x * SIDE + z


def to_row(source, target, send_sem, recv_sem, row):
    return pltpu.make_async_remote_copy(
        src_ref=source,
        dst_ref=target,
        send_sem=send_sem,
        recv_sem=recv_sem,
        device_id={"row": row},
        device_id_type=MESH,
    )


def split(values):
    high = values.astype(BF16)
    low = (values - high.astype(F32)).astype(BF16)
    return high, low


def nt_dot(a, b, precision=None):
    return lax.dot_general(
        a, b, (((1,), (1,)), ((), ())), precision=precision, preferred_element_type=F32
    )


def spread_lane(values, lane):
    return jnp.broadcast_to(values[:, lane : lane + 1], (8, 128))


def spread_row(values, row):
    return jnp.broadcast_to(values[row : row + 1, :], (8, 128))


def factor_in_place(work, meanwhile):
    sub = lax.broadcasted_iota(jnp.int32, (8, 128), 0)
    groups = BLOCK // 8
    for block in range(S // BLOCK):
        base = block * BLOCK
        left = [work[base + 8 * g : base + 8 * g + 8, 0:128] for g in range(groups)]
        right = [work[base + 8 * g : base + 8 * g + 8, 128:256] for g in range(groups)]
        inverted = []
        for panel in range(groups):
            scales = jnp.zeros((8, 128), F32)
            active = range(panel, groups)
            columns = [
                {g: spread_lane(left[g], base + 8 * panel + j) for g in active} for j in range(8)
            ]
            for j in range(8):
                scale = 1.0 / spread_row(columns[j][panel], j)
                scales = jnp.where(sub == j, scale, scales)
                row_left = spread_row(left[panel], j)
                row_right = spread_row(right[panel], j)
                across = {i: spread_row(columns[i][panel], j) for i in range(j + 1, 8)}
                for g in active:
                    multiplier = columns[j][g] * scale
                    if g == panel:
                        multiplier = jnp.where(sub > j, multiplier, 0.0)
                    for i in range(j + 1, 8):
                        columns[i][g] = columns[i][g] - multiplier * across[i]
                    left[g] = left[g] - multiplier * row_left
                    right[g] = right[g] - multiplier * row_right
            inverted.append(scales)
            if meanwhile and panel % 2 == 0:
                meanwhile.pop(0)()
        strip_left = jnp.concatenate(left, axis=0)
        strip_right = jnp.concatenate(right, axis=0)
        work[base : base + BLOCK, 0:128] = strip_left
        work[base : base + BLOCK, 128:256] = strip_right
        after = base + BLOCK
        if after < S:
            lower = strip_left * jnp.concatenate(inverted, axis=0)
            strip = jnp.concatenate([strip_left, strip_right], axis=1)
            product = lax.dot_general(
                lower, strip, (((0,), (0,)), ((), ())), precision=HIGHEST, preferred_element_type=F32
            )
            work[after:S, :] = work[after:S, :] - product[after:S, :]
    while meanwhile:
        meanwhile.pop(0)()


def fronts_kernel(
    child_ref, pivot_ref, update_ref, map_ref, lhat_out, schur_out, share_out,
    maps, near_ref, next_ref, far_ref, panel_ref, hot_ref, high_ref, low_ref, spread_ref, work,
    lhat_ref, rest_ref, added_ref, landed, negative_ref, row_counts, total_ref, column_counts,
    own_sem, in_send, in_recv, out_send, out_recv, count_send, count_recv, row_send, row_recv,
):
    me = lax.axis_index("row")
    col = lax.axis_index("col")
    others = [peer(me, dx, dz) for dx, dz in OFFSETS]
    columns = [lax.rem(col + d, N_COL) for d in range(1, N_COL)]

    barrier = pltpu.get_barrier_semaphore()
    for other in others:
        pl.semaphore_signal(barrier, inc=1, device_id={"row": other}, device_id_type=MESH)
    for other in columns:
        pl.semaphore_signal(barrier, inc=1, device_id={"col": other}, device_id_type=MESH)

    group = me // SIDE
    near = pl.multiple_of(group * 128, 128)
    following = pl.multiple_of(lax.rem(group + 1, 4) * 128, 128)
    opposite = pl.multiple_of(lax.rem(group + 2, 4) * 128, 128)
    far_child = group // 2
    held = pl.ds(pl.multiple_of(me * HELD, HELD), HELD)
    pivot_rows = pl.ds(pl.multiple_of(me * SP, SP), SP)
    update_rows = pl.ds(pl.multiple_of(S + me * UP, SP), UP)

    def pieces(front):
        return (
            (pivot_ref.at[front], panel_ref.at[pivot_rows]),
            (child_ref.at[front, 0, :, pl.ds(near, 128)], near_ref.at[0, held]),
            (child_ref.at[front, 0, :, pl.ds(following, 128)], next_ref.at[0, held]),
            (child_ref.at[front, far_child, :, pl.ds(opposite, 128)], far_ref.at[held]),
            (child_ref.at[front, 1, :, pl.ds(near, 128)], near_ref.at[1, held]),
            (child_ref.at[front, 1, :, pl.ds(following, 128)], next_ref.at[1, held]),
            (update_ref.at[front, :, pl.ds(0, S)], panel_ref.at[update_rows]),
        )

    map_copy = pltpu.make_async_copy(map_ref.at[me], maps, own_sem.at[PIECES])
    map_copy.start()
    own = [
        pltpu.make_async_copy(source, target, own_sem.at[i])
        for i, (source, target) in enumerate(pieces(me))
    ]
    for copy in own:
        copy.start()
    pl.semaphore_wait(barrier, PEERS + N_COL - 1)
    incoming = [
        [
            to_row(*pieces(other)[i], in_send.at[place, i], in_recv.at[place, i], other)
            for place, other in enumerate(others)
        ]
        for i in range(PIECES)
    ]
    for kind in incoming:
        for copy in kind:
            copy.start()

    def arrived(kinds):
        for i in kinds:
            own[i].wait()
            for copy in incoming[i]:
                copy.wait_recv()

    trailing_copy = pltpu.make_async_copy(
        update_ref.at[:, :, pl.ds(S, U)], schur_out, own_sem.at[PIECES + 1]
    )
    trailing_copy.start()
    map_copy.wait()
    for child in range(2):
        indices = maps[child : child + 1, :]
        position = lax.broadcasted_iota(jnp.int32, (F, CU), 0)
        hot_ref[child] = jnp.where(indices == position, 1.0, 0.0).astype(BF16)

    def fill(i, j, block):
        high, low = split(block)
        high_ref[128 * i : 128 * i + 128, 128 * j : 128 * j + 128] = high
        low_ref[128 * i : 128 * i + 128, 128 * j : 128 * j + 128] = low

    def fill_child(child):
        for i in range(4):
            rows = slice(128 * i, 128 * i + 128)
            fill(i, i, near_ref[child, rows, :])
            block = next_ref[child, rows, :]
            fill(i, (i + 1) % 4, block)
            fill((i + 1) % 4, i, block.T)
        for i in (2 * child, 2 * child + 1):
            block = far_ref[128 * i : 128 * i + 128, :]
            fill(i, (i + 2) % 4, block)
            fill((i + 2) % 4, i, block.T)

    def spread_rows(child, first, count):
        for part, ref in enumerate((high_ref, low_ref)):
            spread_ref[child, part, first : first + count, :] = jnp.dot(
                hot_ref[child, first : first + count, :], ref[...], preferred_element_type=F32
            ).astype(BF16)

    def placed(start, size, first, count):
        total = None
        for child in range(2):
            hot = hot_ref[child, start : start + size, :]
            for part in range(2):
                term = nt_dot(spread_ref[child, part, first : first + count, :], hot)
                total = term if total is None else total + term
        return total

    arrived((0, 1, 2, 3))
    fill_child(0)
    spread_rows(0, 0, F)
    arrived((4, 5))
    fill_child(1)
    spread_rows(1, 0, S)
    lane = lax.broadcasted_iota(jnp.int32, (S, S), 1)
    place = lax.broadcasted_iota(jnp.int32, (S, S), 0)
    work[:, 0:128] = panel_ref[0:S, :] + placed(0, S, 0, S)
    work[:, 128:256] = jnp.where(lane == place, 1.0, 0.0)

    def spread_later(first):
        return lambda: spread_rows(1, first, 320)

    def placed_later(start, first):
        def run():
            block = placed(start, 256, first, 320)
            rows = slice(first - S, first - S + 320)
            if start == 0:
                added_ref[rows, :] = block[:, 0:128]
                rest_ref[rows, 0:128] = block[:, 128:256]
            else:
                rest_ref[rows, start - S : start - S + 256] = block
        return run

    halves = (S, S + 320)
    factor_in_place(
        work,
        [spread_later(first) for first in halves]
        + [placed_later(start, first) for start in (0, 256, 512) for first in halves],
    )
    inverse = work[:, 128:256]
    pivots = jnp.sum(jnp.where(lane == place, work[:, 0:128], 0.0), axis=0, keepdims=True)
    negative = jnp.where(pivots < 0.0, 1.0, 0.0)
    negative_ref[0] = negative
    row_counts[me] = negative
    tallies = [
        to_row(negative_ref.at[0], row_counts.at[me], row_send.at[i], row_recv.at[i], other)
        for i, other in enumerate(others)
    ]
    for copy in tallies:
        copy.start()
    arrived((6,))
    lhat = nt_dot(panel_ref[S:, :] + added_ref[...], inverse, HIGHEST)
    lhat_ref[...] = lhat

    def share(row):
        return pl.ds(pl.multiple_of(row * UP, SP), UP)

    outgoing = [
        [
            to_row(
                source.at[share(other)], target.at[me], out_send.at[i, kind], out_recv.at[i, kind], other
            )
            for i, other in enumerate(others)
        ]
        for kind, (source, target) in enumerate(((lhat_ref, lhat_out), (rest_ref, landed)))
    ]
    for copy in outgoing[0]:
        copy.start()
    scaled = lhat / pivots
    for start, size in ((0, 256), (256, 256), (512, 128)):
        correction = nt_dot(scaled, lhat[start : start + size], HIGHEST)
        rest_ref[:, start : start + size] = rest_ref[:, start : start + size] - correction
    for copy in outgoing[1]:
        copy.start()
    lhat_out[me] = lhat_ref[share(me), :]
    for copy in tallies:
        copy.wait()
    row_total = jnp.sum(row_counts[...], axis=0)
    total_ref[0] = row_total
    column_counts[col] = row_total
    trailing_copy.wait()
    schur_out[me] = schur_out[me] + rest_ref[share(me), :]
    forwards = [
        pltpu.make_async_remote_copy(
            src_ref=total_ref.at[0],
            dst_ref=column_counts.at[col],
            send_sem=count_send.at[i],
            recv_sem=count_recv.at[i],
            device_id={"col": other},
            device_id_type=MESH,
        )
        for i, other in enumerate(columns)
    ]
    for copy in forwards:
        copy.start()
    for i, (dx, dz) in enumerate(OFFSETS):
        outgoing[1][i].wait_recv()
        source = peer(me, (SIDE - dx) % SIDE, (SIDE - dz) % SIDE)
        schur_out[source] = schur_out[source] + landed[source]
        if i == PEERS // 2:
            for copy in forwards:
                copy.wait()
            flat = jnp.sum(column_counts[...], axis=0)
            share_out[...] = jnp.sum(flat, axis=1, keepdims=True) / float(N_ROW * N_COL * S)
    for copy in outgoing[0]:
        copy.wait()
    for copy in outgoing[1]:
        copy.wait_send()
    for kind in incoming:
        for copy in kind:
            copy.wait_send()


def fronts(child_blocks, front_pivot, front_update, child_map):
    any_spec = pl.BlockSpec(memory_space=pl.ANY)
    vmem_spec = pl.BlockSpec(memory_space=pltpu.VMEM)
    dma = pltpu.SemaphoreType.DMA
    return pl.pallas_call(
        fronts_kernel,
        out_shape=(
            pltpu.VMEM((N_ROW, UP, S), F32),
            pltpu.VMEM((N_ROW, UP, U), F32),
            jax.ShapeDtypeStruct((1, 1), F32),
        ),
        in_specs=[any_spec] * 4,
        out_specs=(vmem_spec, vmem_spec, vmem_spec),
        scratch_shapes=[
            pltpu.VMEM((2, CU), jnp.int32),
            pltpu.VMEM((2, CU, 128), F32),
            pltpu.VMEM((2, CU, 128), F32),
            pltpu.VMEM((CU, 128), F32),
            pltpu.VMEM((F, S), F32),
            pltpu.VMEM((2, F, CU), BF16),
            pltpu.VMEM((CU, CU), BF16),
            pltpu.VMEM((CU, CU), BF16),
            pltpu.VMEM((2, 2, F, CU), BF16),
            pltpu.VMEM((S, 2 * S), F32),
            pltpu.VMEM((U, S), F32),
            pltpu.VMEM((U, U), F32),
            pltpu.VMEM((U, S), F32),
            pltpu.VMEM((N_ROW, UP, U), F32),
            pltpu.VMEM((1, 1, S), F32),
            pltpu.VMEM((N_ROW, 1, S), F32),
            pltpu.VMEM((1, 1, S), F32),
            pltpu.VMEM((N_COL, 1, S), F32),
            dma((PIECES + 2,)),
            dma((PEERS, PIECES)),
            dma((PEERS, PIECES)),
            dma((PEERS, 2)),
            dma((PEERS, 2)),
            dma((N_COL - 1,)),
            dma((N_COL - 1,)),
            dma((PEERS,)),
            dma((PEERS,)),
        ],
        compiler_params=pltpu.CompilerParams(collective_id=0, has_side_effects=True),
        name="fronts",
    )(child_blocks, front_pivot, front_update, child_map)


def store_kernel(lhat_ref, schur_ref, lhat_out, schur_out, sem):
    copies = [pltpu.make_async_copy(lhat_ref, lhat_out, sem.at[N_ROW])]
    for i in range(N_ROW):
        copies.append(pltpu.make_async_copy(schur_ref.at[i], schur_out.at[i], sem.at[i]))
    for copy in copies:
        copy.start()
    for copy in copies:
        copy.wait()


def store(lhat, schur):
    any_spec = pl.BlockSpec(memory_space=pl.ANY)
    vmem_spec = pl.BlockSpec(memory_space=pltpu.VMEM)
    return pl.pallas_call(
        store_kernel,
        out_shape=(
            jax.ShapeDtypeStruct(lhat.shape, F32),
            jax.ShapeDtypeStruct(schur.shape, F32),
        ),
        in_specs=[vmem_spec] * 2,
        out_specs=(any_spec,) * 2,
        scratch_shapes=[pltpu.SemaphoreType.DMA((N_ROW + 1,))],
        compiler_params=pltpu.CompilerParams(vmem_limit_bytes=1 << 20),
        name="store",
    )(lhat, schur)


def local(front_pivot, front_update, child_blocks, child_map):
    lhat, schur, share = fronts(child_blocks, front_pivot, front_update, child_map)
    lhat, schur = store(lhat, schur)
    return (lhat, schur, share[0, 0])


def solution(mesh):
    in_specs = (
        P("col", "row", None),
        P("col", "row", None),
        P("col", None, "row", None),
        P("col", None, None),
    )
    out_specs = (P("col", "row", None), P("col", "row", None), P())
    return jax.shard_map(local, mesh=mesh, in_specs=in_specs, out_specs=out_specs, check_vma=False)
```

```python
import jax
import jax.numpy as jnp
from jax import lax
from jax.experimental import pallas as pl
from jax.experimental.pallas import tpu as pltpu
from jax.sharding import PartitionSpec as P

MESH = pl.DeviceIdType.MESH
F32 = jnp.float32
BF16 = jnp.bfloat16
HIGHEST = lax.Precision.HIGHEST

N_ROW = 16
N_COL = 8
SIDE = 4
S = 128
CU = 512
U = 640
F = 768
SP = 8
UP = 40
HELD = 32
BLOCK = 64
ALL = [(dx, (dx + t) % 4) for t in range(4) for dx in range(4) if (dx, (dx + t) % 4) != (0, 0)]
OFFSETS = ALL
PEERS = len(OFFSETS)
PIECES = 7


def peer(me, dx, dz):
    x = lax.rem(me // SIDE + dx, SIDE)
    z = lax.rem(lax.rem(me, SIDE) + dz, SIDE)
    return x * SIDE + z


def to_row(source, target, send_sem, recv_sem, row):
    return pltpu.make_async_remote_copy(
        src_ref=source,
        dst_ref=target,
        send_sem=send_sem,
        recv_sem=recv_sem,
        device_id={"row": row},
        device_id_type=MESH,
    )


def split(values):
    high = values.astype(BF16)
    low = (values - high.astype(F32)).astype(BF16)
    return high, low


def nt_dot(a, b, precision=None):
    return lax.dot_general(
        a, b, (((1,), (1,)), ((), ())), precision=precision, preferred_element_type=F32
    )


def spread_lane(values, lane):
    return jnp.broadcast_to(values[:, lane : lane + 1], (8, 128))


def spread_row(values, row):
    return jnp.broadcast_to(values[row : row + 1, :], (8, 128))


def factor_in_place(work, meanwhile):
    sub = lax.broadcasted_iota(jnp.int32, (8, 128), 0)
    groups = BLOCK // 8
    for block in range(S // BLOCK):
        base = block * BLOCK
        left = [work[base + 8 * g : base + 8 * g + 8, 0:128] for g in range(groups)]
        right = [work[base + 8 * g : base + 8 * g + 8, 128:256] for g in range(groups)]
        inverted = []
        for panel in range(groups):
            scales = jnp.zeros((8, 128), F32)
            active = range(panel, groups)
            columns = [
                {g: spread_lane(left[g], base + 8 * panel + j) for g in active} for j in range(8)
            ]
            for j in range(8):
                scale = 1.0 / spread_row(columns[j][panel], j)
                scales = jnp.where(sub == j, scale, scales)
                row_left = spread_row(left[panel], j)
                row_right = spread_row(right[panel], j)
                across = {i: spread_row(columns[i][panel], j) for i in range(j + 1, 8)}
                for g in active:
                    multiplier = columns[j][g] * scale
                    if g == panel:
                        multiplier = jnp.where(sub > j, multiplier, 0.0)
                    for i in range(j + 1, 8):
                        columns[i][g] = columns[i][g] - multiplier * across[i]
                    left[g] = left[g] - multiplier * row_left
                    right[g] = right[g] - multiplier * row_right
            inverted.append(scales)
            if meanwhile and panel % 2 == 0:
                meanwhile.pop(0)()
        strip_left = jnp.concatenate(left, axis=0)
        strip_right = jnp.concatenate(right, axis=0)
        work[base : base + BLOCK, 0:128] = strip_left
        work[base : base + BLOCK, 128:256] = strip_right
        after = base + BLOCK
        if after < S:
            lower = strip_left * jnp.concatenate(inverted, axis=0)
            strip = jnp.concatenate([strip_left, strip_right], axis=1)
            product = lax.dot_general(
                lower, strip, (((0,), (0,)), ((), ())), precision=HIGHEST, preferred_element_type=F32
            )
            work[after:S, :] = work[after:S, :] - product[after:S, :]
    while meanwhile:
        meanwhile.pop(0)()


def fronts_kernel(
    child_ref, pivot_ref, update_ref, map_ref, lhat_out, schur_out, share_out,
    maps, near_ref, next_ref, far_ref, panel_ref, hot_ref, high_ref, low_ref, spread_ref, work,
    lhat_ref, rest_ref, added_ref, landed, negative_ref, row_counts, total_ref, column_counts,
    own_sem, in_send, in_recv, out_send, out_recv, count_send, count_recv, row_send, row_recv,
):
    me = lax.axis_index("row")
    col = lax.axis_index("col")
    others = [peer(me, dx, dz) for dx, dz in OFFSETS]
    columns = [lax.rem(col + d, N_COL) for d in range(1, N_COL)]

    barrier = pltpu.get_barrier_semaphore()
    for other in others:
        pl.semaphore_signal(barrier, inc=1, device_id={"row": other}, device_id_type=MESH)
    for other in columns:
        pl.semaphore_signal(barrier, inc=1, device_id={"col": other}, device_id_type=MESH)

    group = me // SIDE
    near = pl.multiple_of(group * 128, 128)
    following = pl.multiple_of(lax.rem(group + 1, 4) * 128, 128)
    opposite = pl.multiple_of(lax.rem(group + 2, 4) * 128, 128)
    far_child = group // 2
    held = pl.ds(pl.multiple_of(me * HELD, HELD), HELD)
    pivot_rows = pl.ds(pl.multiple_of(me * SP, SP), SP)
    update_rows = pl.ds(pl.multiple_of(S + me * UP, SP), UP)

    def pieces(front):
        return (
            (pivot_ref.at[front], panel_ref.at[pivot_rows]),
            (child_ref.at[front, 0, :, pl.ds(near, 128)], near_ref.at[0, held]),
            (child_ref.at[front, 0, :, pl.ds(following, 128)], next_ref.at[0, held]),
            (child_ref.at[front, far_child, :, pl.ds(opposite, 128)], far_ref.at[held]),
            (child_ref.at[front, 1, :, pl.ds(near, 128)], near_ref.at[1, held]),
            (child_ref.at[front, 1, :, pl.ds(following, 128)], next_ref.at[1, held]),
            (update_ref.at[front, :, pl.ds(0, S)], panel_ref.at[update_rows]),
        )

    map_copy = pltpu.make_async_copy(map_ref.at[me], maps, own_sem.at[PIECES])
    map_copy.start()
    own = [
        pltpu.make_async_copy(source, target, own_sem.at[i])
        for i, (source, target) in enumerate(pieces(me))
    ]
    for copy in own:
        copy.start()
    pl.semaphore_wait(barrier, PEERS + N_COL - 1)
    incoming = [
        [
            to_row(*pieces(other)[i], in_send.at[place, i], in_recv.at[place, i], other)
            for place, other in enumerate(others)
        ]
        for i in range(PIECES)
    ]
    for kind in incoming:
        for copy in kind:
            copy.start()

    def arrived(kinds):
        for i in kinds:
            own[i].wait()
            for copy in incoming[i]:
                copy.wait_recv()

    trailing_copy = pltpu.make_async_copy(
        update_ref.at[:, :, pl.ds(S, U)], schur_out, own_sem.at[PIECES + 1]
    )
    trailing_copy.start()
    map_copy.wait()
    for child in range(2):
        indices = maps[child : child + 1, :]
        position = lax.broadcasted_iota(jnp.int32, (F, CU), 0)
        hot_ref[child] = jnp.where(indices == position, 1.0, 0.0).astype(BF16)

    def fill(i, j, block):
        high, low = split(block)
        high_ref[128 * i : 128 * i + 128, 128 * j : 128 * j + 128] = high
        low_ref[128 * i : 128 * i + 128, 128 * j : 128 * j + 128] = low

    def fill_child(child):
        for i in range(4):
            rows = slice(128 * i, 128 * i + 128)
            fill(i, i, near_ref[child, rows, :])
            block = next_ref[child, rows, :]
            fill(i, (i + 1) % 4, block)
            fill((i + 1) % 4, i, block.T)
        for i in (2 * child, 2 * child + 1):
            block = far_ref[128 * i : 128 * i + 128, :]
            fill(i, (i + 2) % 4, block)
            fill((i + 2) % 4, i, block.T)

    def spread_rows(child, first, count):
        for part, ref in enumerate((high_ref, low_ref)):
            spread_ref[child, part, first : first + count, :] = jnp.dot(
                hot_ref[child, first : first + count, :], ref[...], preferred_element_type=F32
            ).astype(BF16)

    def placed(start, size, first, count):
        total = None
        for child in range(2):
            hot = hot_ref[child, start : start + size, :]
            for part in range(2):
                term = nt_dot(spread_ref[child, part, first : first + count, :], hot)
                total = term if total is None else total + term
        return total

    arrived((0, 1, 2, 3))
    fill_child(0)
    spread_rows(0, 0, F)
    arrived((4, 5))
    fill_child(1)
    spread_rows(1, 0, S)
    lane = lax.broadcasted_iota(jnp.int32, (S, S), 1)
    place = lax.broadcasted_iota(jnp.int32, (S, S), 0)
    work[:, 0:128] = panel_ref[0:S, :] + placed(0, S, 0, S)
    work[:, 128:256] = jnp.where(lane == place, 1.0, 0.0)

    def spread_later(first):
        return lambda: spread_rows(1, first, 320)

    def placed_later(start, first):
        def run():
            block = placed(start, 256, first, 320)
            rows = slice(first - S, first - S + 320)
            if start == 0:
                added_ref[rows, :] = block[:, 0:128]
                rest_ref[rows, 0:128] = block[:, 128:256]
            else:
                rest_ref[rows, start - S : start - S + 256] = block
        return run

    halves = (S, S + 320)
    factor_in_place(
        work,
        [spread_later(first) for first in halves]
        + [placed_later(start, first) for start in (0, 256, 512) for first in halves],
    )
    inverse = work[:, 128:256]
    pivots = jnp.sum(jnp.where(lane == place, work[:, 0:128], 0.0), axis=0, keepdims=True)
    negative = jnp.where(pivots < 0.0, 1.0, 0.0)
    negative_ref[0] = negative
    row_counts[me] = negative
    tallies = [
        to_row(negative_ref.at[0], row_counts.at[me], row_send.at[i], row_recv.at[i], other)
        for i, other in enumerate(others)
    ]
    for copy in tallies:
        copy.start()
    arrived((6,))
    lhat = nt_dot(panel_ref[S:, :] + added_ref[...], inverse, HIGHEST)
    lhat_ref[...] = lhat

    def share(row):
        return pl.ds(pl.multiple_of(row * UP, SP), UP)

    outgoing = [
        [
            to_row(
                source.at[share(other)], target.at[me], out_send.at[i, kind], out_recv.at[i, kind], other
            )
            for i, other in enumerate(others)
        ]
        for kind, (source, target) in enumerate(((lhat_ref, lhat_out), (rest_ref, landed)))
    ]
    for copy in outgoing[0]:
        copy.start()
    scaled = lhat / pivots
    for start, size in ((0, 256), (256, 256), (512, 128)):
        correction = nt_dot(scaled, lhat[start : start + size], HIGHEST)
        rest_ref[:, start : start + size] = rest_ref[:, start : start + size] - correction
    for copy in outgoing[1]:
        copy.start()
    lhat_out[me] = lhat_ref[share(me), :]
    for copy in tallies:
        copy.wait()
    row_total = jnp.sum(row_counts[...], axis=0)
    total_ref[0] = row_total
    column_counts[col] = row_total
    trailing_copy.wait()
    schur_out[me] = schur_out[me] + rest_ref[share(me), :]
    forwards = [
        pltpu.make_async_remote_copy(
            src_ref=total_ref.at[0],
            dst_ref=column_counts.at[col],
            send_sem=count_send.at[i],
            recv_sem=count_recv.at[i],
            device_id={"col": other},
            device_id_type=MESH,
        )
        for i, other in enumerate(columns)
    ]
    for copy in forwards:
        copy.start()
    for i, (dx, dz) in enumerate(OFFSETS):
        outgoing[1][i].wait_recv()
        source = peer(me, (SIDE - dx) % SIDE, (SIDE - dz) % SIDE)
        schur_out[source] = schur_out[source] + landed[source]
        if i == PEERS // 2:
            for copy in forwards:
                copy.wait()
            flat = jnp.sum(column_counts[...], axis=0)
            share_out[...] = jnp.sum(flat, axis=1, keepdims=True) / float(N_ROW * N_COL * S)
    for copy in outgoing[0]:
        copy.wait()
    for copy in outgoing[1]:
        copy.wait_send()
    for kind in incoming:
        for copy in kind:
            copy.wait_send()


def fronts(child_blocks, front_pivot, front_update, child_map):
    any_spec = pl.BlockSpec(memory_space=pl.ANY)
    vmem_spec = pl.BlockSpec(memory_space=pltpu.VMEM)
    dma = pltpu.SemaphoreType.DMA
    return pl.pallas_call(
        fronts_kernel,
        out_shape=(
            pltpu.VMEM((N_ROW, UP, S), F32),
            pltpu.VMEM((N_ROW, UP, U), F32),
            jax.ShapeDtypeStruct((1, 1), F32),
        ),
        in_specs=[any_spec] * 4,
        out_specs=(vmem_spec, vmem_spec, vmem_spec),
        scratch_shapes=[
            pltpu.VMEM((2, CU), jnp.int32),
            pltpu.VMEM((2, CU, 128), F32),
            pltpu.VMEM((2, CU, 128), F32),
            pltpu.VMEM((CU, 128), F32),
            pltpu.VMEM((F, S), F32),
            pltpu.VMEM((2, F, CU), BF16),
            pltpu.VMEM((CU, CU), BF16),
            pltpu.VMEM((CU, CU), BF16),
            pltpu.VMEM((2, 2, F, CU), BF16),
            pltpu.VMEM((S, 2 * S), F32),
            pltpu.VMEM((U, S), F32),
            pltpu.VMEM((U, U), F32),
            pltpu.VMEM((U, S), F32),
            pltpu.VMEM((N_ROW, UP, U), F32),
            pltpu.VMEM((1, 1, S), F32),
            pltpu.VMEM((N_ROW, 1, S), F32),
            pltpu.VMEM((1, 1, S), F32),
            pltpu.VMEM((N_COL, 1, S), F32),
            dma((PIECES + 2,)),
            dma((PEERS, PIECES)),
            dma((PEERS, PIECES)),
            dma((PEERS, 2)),
            dma((PEERS, 2)),
            dma((N_COL - 1,)),
            dma((N_COL - 1,)),
            dma((PEERS,)),
            dma((PEERS,)),
        ],
        compiler_params=pltpu.CompilerParams(collective_id=0, has_side_effects=True),
        name="fronts",
    )(child_blocks, front_pivot, front_update, child_map)


def store_kernel(lhat_ref, schur_ref, lhat_out, schur_out, sem):
    copies = [pltpu.make_async_copy(lhat_ref, lhat_out, sem.at[N_ROW])]
    for i in range(N_ROW):
        copies.append(pltpu.make_async_copy(schur_ref.at[i], schur_out.at[i], sem.at[i]))
    for copy in copies:
        copy.start()
    for copy in copies:
        copy.wait()


def store(lhat, schur):
    any_spec = pl.BlockSpec(memory_space=pl.ANY)
    vmem_spec = pl.BlockSpec(memory_space=pltpu.VMEM)
    return pl.pallas_call(
        store_kernel,
        out_shape=(
            jax.ShapeDtypeStruct(lhat.shape, F32),
            jax.ShapeDtypeStruct(schur.shape, F32),
        ),
        in_specs=[vmem_spec] * 2,
        out_specs=(any_spec,) * 2,
        scratch_shapes=[pltpu.SemaphoreType.DMA((N_ROW + 1,))],
        compiler_params=pltpu.CompilerParams(vmem_limit_bytes=1 << 20),
        name="store",
    )(lhat, schur)


def local(front_pivot, front_update, child_blocks, child_map):
    lhat, schur, share = fronts(child_blocks, front_pivot, front_update, child_map)
    lhat, schur = store(lhat, schur)
    return (lhat, schur, share[0, 0])


def solution(mesh):
    in_specs = (
        P("col", "row", None),
        P("col", "row", None),
        P("col", None, "row", None),
        P("col", None, None),
    )
    out_specs = (P("col", "row", None), P("col", "row", None), P())
    return jax.shard_map(local, mesh=mesh, in_specs=in_specs, out_specs=out_specs, check_vma=False)
```

```python
import jax
import jax.numpy as jnp
from jax import lax
from jax.experimental import pallas as pl
from jax.experimental.pallas import tpu as pltpu
from jax.sharding import PartitionSpec as P

MESH = pl.DeviceIdType.MESH
F32 = jnp.float32
BF16 = jnp.bfloat16
HIGHEST = lax.Precision.HIGHEST

N_ROW = 16
N_COL = 8
SIDE = 4
S = 128
CU = 512
U = 640
F = 768
SP = 8
UP = 40
HELD = 32
BLOCK = 64
ALL = [(dx, (dx + t) % 4) for t in range(4) for dx in range(4) if (dx, (dx + t) % 4) != (0, 0)]
OFFSETS = ALL
PEERS = len(OFFSETS)
PIECES = 7


def peer(me, dx, dz):
    x = lax.rem(me // SIDE + dx, SIDE)
    z = lax.rem(lax.rem(me, SIDE) + dz, SIDE)
    return x * SIDE + z


def to_row(source, target, send_sem, recv_sem, row):
    return pltpu.make_async_remote_copy(
        src_ref=source,
        dst_ref=target,
        send_sem=send_sem,
        recv_sem=recv_sem,
        device_id={"row": row},
        device_id_type=MESH,
    )


def split(values):
    high = values.astype(BF16)
    low = (values - high.astype(F32)).astype(BF16)
    return high, low


def nt_dot(a, b, precision=None):
    return lax.dot_general(
        a, b, (((1,), (1,)), ((), ())), precision=precision, preferred_element_type=F32
    )


def spread_lane(values, lane):
    return jnp.broadcast_to(values[:, lane : lane + 1], (8, 128))


def spread_row(values, row):
    return jnp.broadcast_to(values[row : row + 1, :], (8, 128))


def factor_in_place(work, meanwhile):
    sub = lax.broadcasted_iota(jnp.int32, (8, 128), 0)
    groups = BLOCK // 8
    for block in range(S // BLOCK):
        base = block * BLOCK
        left = [work[base + 8 * g : base + 8 * g + 8, 0:128] for g in range(groups)]
        right = [work[base + 8 * g : base + 8 * g + 8, 128:256] for g in range(groups)]
        inverted = []
        for panel in range(groups):
            scales = jnp.zeros((8, 128), F32)
            active = range(panel, groups)
            columns = [
                {g: spread_lane(left[g], base + 8 * panel + j) for g in active} for j in range(8)
            ]
            for j in range(8):
                scale = 1.0 / spread_row(columns[j][panel], j)
                scales = jnp.where(sub == j, scale, scales)
                row_left = spread_row(left[panel], j)
                row_right = spread_row(right[panel], j)
                across = {i: spread_row(columns[i][panel], j) for i in range(j + 1, 8)}
                for g in active:
                    multiplier = columns[j][g] * scale
                    if g == panel:
                        multiplier = jnp.where(sub > j, multiplier, 0.0)
                    for i in range(j + 1, 8):
                        columns[i][g] = columns[i][g] - multiplier * across[i]
                    left[g] = left[g] - multiplier * row_left
                    right[g] = right[g] - multiplier * row_right
            inverted.append(scales)
            if meanwhile and panel % 2 == 0:
                meanwhile.pop(0)()
        strip_left = jnp.concatenate(left, axis=0)
        strip_right = jnp.concatenate(right, axis=0)
        work[base : base + BLOCK, 0:128] = strip_left
        work[base : base + BLOCK, 128:256] = strip_right
        after = base + BLOCK
        if after < S:
            lower = strip_left * jnp.concatenate(inverted, axis=0)
            strip = jnp.concatenate([strip_left, strip_right], axis=1)
            product = lax.dot_general(
                lower, strip, (((0,), (0,)), ((), ())), precision=HIGHEST, preferred_element_type=F32
            )
            work[after:S, :] = work[after:S, :] - product[after:S, :]
    while meanwhile:
        meanwhile.pop(0)()


def turned(values, shift):
    shift %= 128
    if shift == 0:
        return values
    return jnp.concatenate([values[:, 128 - shift :], values[:, : 128 - shift]], axis=1)


def pack(near_src, packed_src, extra_src, quarter):
    which = jnp.full((HELD, 128), quarter, jnp.int32)
    lane = lax.broadcasted_iota(jnp.int32, (HELD, 128), 1)

    def one(front, carry):
        aligned = []
        for child in range(2):
            strip = near_src[front, child]
            result = strip
            for q in range(1, 4):
                result = jnp.where(which == q, turned(strip, -32 * q), result)
            aligned.append(result)
        packed_src[front] = jnp.where(lane < 64, aligned[0], turned(aligned[1], 64))
        chosen = jnp.where(which < 2, aligned[0], aligned[1])
        extra = turned(chosen[0:8], -64)
        for q in range(1, 4):
            moved = turned(chosen[8 * q : 8 * q + 8], 32 * q - 64)
            extra = jnp.where(lane[0:8] // 32 == q, moved, extra)
        extra_src[front] = extra
        return carry

    lax.fori_loop(0, N_ROW, one, 0)


def unpack(near_ref, extra_ref, child, group):
    lane = lax.broadcasted_iota(jnp.int32, (8, 128), 1) // 32
    rows = []
    for s in range(4):
        source = 4 * group + s
        strip = near_ref[32 * source : 32 * source + 32, :]
        strip = turned(strip, 32 * s - 64 * child)
        if s // 2 == child:
            extra = extra_ref[8 * source : 8 * source + 8, :]
            for q in range(4):
                moved = turned(extra, 32 * ((s + 2) % 4) - 32 * q)
                rows.append(jnp.where(lane == (s + 2) % 4, moved, strip[8 * q : 8 * q + 8]))
        else:
            rows.append(strip)
    half = jnp.concatenate(rows, axis=0)
    above = lax.broadcasted_iota(jnp.int32, (128, 128), 0) // 32
    ahead = (lax.broadcasted_iota(jnp.int32, (128, 128), 1) // 32 - above + 4) % 4
    kept = (ahead < 2) | ((ahead == 2) & (above // 2 == child))
    return jnp.where(kept, half, half.T)


def fronts_kernel(
    child_ref, pivot_ref, update_ref, map_ref, lhat_out, schur_out, share_out,
    maps, near_src, packed_src, extra_src, near_ref, extra_ref, next_ref, far_ref, panel_ref, hot_ref, high_ref, low_ref, spread_ref, work,
    lhat_ref, rest_ref, added_ref, landed, negative_ref, row_counts, total_ref, column_counts,
    own_sem, in_send, in_recv, out_send, out_recv, count_send, count_recv, row_send, row_recv,
):
    me = lax.axis_index("row")
    col = lax.axis_index("col")
    others = [peer(me, dx, dz) for dx, dz in OFFSETS]
    columns = [lax.rem(col + d, N_COL) for d in range(1, N_COL)]

    barrier = pltpu.get_barrier_semaphore()
    for other in others:
        pl.semaphore_signal(barrier, inc=1, device_id={"row": other}, device_id_type=MESH)
    for other in columns:
        pl.semaphore_signal(barrier, inc=1, device_id={"col": other}, device_id_type=MESH)

    group = me // SIDE
    near = pl.multiple_of(group * 128, 128)
    following = pl.multiple_of(lax.rem(group + 1, 4) * 128, 128)
    opposite = pl.multiple_of(lax.rem(group + 2, 4) * 128, 128)
    far_child = group // 2
    held = pl.ds(pl.multiple_of(me * HELD, HELD), HELD)
    pivot_rows = pl.ds(pl.multiple_of(me * SP, SP), SP)
    update_rows = pl.ds(pl.multiple_of(S + me * UP, SP), UP)

    extra_rows = pl.ds(pl.multiple_of(me * 8, 8), 8)

    def pieces(front):
        return (
            (pivot_ref.at[front], panel_ref.at[pivot_rows]),
            (packed_src.at[front], near_ref.at[held]),
            (extra_src.at[front], extra_ref.at[extra_rows]),
            (child_ref.at[front, 0, :, pl.ds(following, 128)], next_ref.at[0, held]),
            (child_ref.at[front, far_child, :, pl.ds(opposite, 128)], far_ref.at[held]),
            (child_ref.at[front, 1, :, pl.ds(following, 128)], next_ref.at[1, held]),
            (update_ref.at[front, :, pl.ds(0, S)], panel_ref.at[update_rows]),
        )

    near_copy = pltpu.make_async_copy(
        child_ref.at[:, :, :, pl.ds(near, 128)], near_src, own_sem.at[PIECES + 2]
    )
    near_copy.start()
    map_copy = pltpu.make_async_copy(map_ref.at[me], maps, own_sem.at[PIECES])
    map_copy.start()
    own = [
        pltpu.make_async_copy(source, target, own_sem.at[i])
        for i, (source, target) in enumerate(pieces(me))
    ]
    near_copy.wait()
    pack(near_src, packed_src, extra_src, lax.rem(me, 4))
    for copy in own:
        copy.start()
    pl.semaphore_wait(barrier, PEERS + N_COL - 1)
    incoming = [
        [
            to_row(*pieces(other)[i], in_send.at[place, i], in_recv.at[place, i], other)
            for place, other in enumerate(others)
        ]
        for i in range(PIECES)
    ]
    for kind in incoming:
        for copy in kind:
            copy.start()

    def arrived(kinds):
        for i in kinds:
            own[i].wait()
            for copy in incoming[i]:
                copy.wait_recv()

    trailing_copy = pltpu.make_async_copy(
        update_ref.at[:, :, pl.ds(S, U)], schur_out, own_sem.at[PIECES + 1]
    )
    trailing_copy.start()
    map_copy.wait()
    for child in range(2):
        indices = maps[child : child + 1, :]
        position = lax.broadcasted_iota(jnp.int32, (F, CU), 0)
        hot_ref[child] = jnp.where(indices == position, 1.0, 0.0).astype(BF16)

    def fill(i, j, block):
        high, low = split(block)
        high_ref[128 * i : 128 * i + 128, 128 * j : 128 * j + 128] = high
        low_ref[128 * i : 128 * i + 128, 128 * j : 128 * j + 128] = low

    def fill_near(child):
        for i in range(4):
            fill(i, i, unpack(near_ref, extra_ref, child, i))

    def fill_child(child):
        for i in range(4):
            rows = slice(128 * i, 128 * i + 128)
            block = next_ref[child, rows, :]
            fill(i, (i + 1) % 4, block)
            fill((i + 1) % 4, i, block.T)
        for i in (2 * child, 2 * child + 1):
            block = far_ref[128 * i : 128 * i + 128, :]
            fill(i, (i + 2) % 4, block)
            fill((i + 2) % 4, i, block.T)

    def spread_rows(child, first, count):
        for part, ref in enumerate((high_ref, low_ref)):
            spread_ref[child, part, first : first + count, :] = jnp.dot(
                hot_ref[child, first : first + count, :], ref[...], preferred_element_type=F32
            ).astype(BF16)

    def placed(start, size, first, count):
        total = None
        for child in range(2):
            hot = hot_ref[child, start : start + size, :]
            for part in range(2):
                term = nt_dot(spread_ref[child, part, first : first + count, :], hot)
                total = term if total is None else total + term
        return total

    arrived((0, 1, 2, 3, 4))
    fill_near(0)
    fill_child(0)
    spread_rows(0, 0, F)
    fill_near(1)
    arrived((5,))
    fill_child(1)
    spread_rows(1, 0, S)
    lane = lax.broadcasted_iota(jnp.int32, (S, S), 1)
    place = lax.broadcasted_iota(jnp.int32, (S, S), 0)
    work[:, 0:128] = panel_ref[0:S, :] + placed(0, S, 0, S)
    work[:, 128:256] = jnp.where(lane == place, 1.0, 0.0)

    def spread_later(first):
        return lambda: spread_rows(1, first, 320)

    def placed_later(start, first):
        def run():
            block = placed(start, 256, first, 320)
            rows = slice(first - S, first - S + 320)
            if start == 0:
                added_ref[rows, :] = block[:, 0:128]
                rest_ref[rows, 0:128] = block[:, 128:256]
            else:
                rest_ref[rows, start - S : start - S + 256] = block
        return run

    halves = (S, S + 320)
    factor_in_place(
        work,
        [spread_later(first) for first in halves]
        + [placed_later(start, first) for start in (0, 256, 512) for first in halves],
    )
    inverse = work[:, 128:256]
    pivots = jnp.sum(jnp.where(lane == place, work[:, 0:128], 0.0), axis=0, keepdims=True)
    negative = jnp.where(pivots < 0.0, 1.0, 0.0)
    negative_ref[0] = negative
    row_counts[me] = negative
    tallies = [
        to_row(negative_ref.at[0], row_counts.at[me], row_send.at[i], row_recv.at[i], other)
        for i, other in enumerate(others)
    ]
    for copy in tallies:
        copy.start()
    arrived((6,))
    lhat = nt_dot(panel_ref[S:, :] + added_ref[...], inverse, HIGHEST)
    lhat_ref[...] = lhat

    def share(row):
        return pl.ds(pl.multiple_of(row * UP, SP), UP)

    outgoing = [
        [
            to_row(
                source.at[share(other)], target.at[me], out_send.at[i, kind], out_recv.at[i, kind], other
            )
            for i, other in enumerate(others)
        ]
        for kind, (source, target) in enumerate(((lhat_ref, lhat_out), (rest_ref, landed)))
    ]
    for copy in outgoing[0]:
        copy.start()
    scaled = lhat / pivots
    for start, size in ((0, 256), (256, 256), (512, 128)):
        correction = nt_dot(scaled, lhat[start : start + size], HIGHEST)
        rest_ref[:, start : start + size] = rest_ref[:, start : start + size] - correction
    for copy in outgoing[1]:
        copy.start()
    lhat_out[me] = lhat_ref[share(me), :]
    for copy in tallies:
        copy.wait()
    row_total = jnp.sum(row_counts[...], axis=0)
    total_ref[0] = row_total
    column_counts[col] = row_total
    trailing_copy.wait()
    schur_out[me] = schur_out[me] + rest_ref[share(me), :]
    forwards = [
        pltpu.make_async_remote_copy(
            src_ref=total_ref.at[0],
            dst_ref=column_counts.at[col],
            send_sem=count_send.at[i],
            recv_sem=count_recv.at[i],
            device_id={"col": other},
            device_id_type=MESH,
        )
        for i, other in enumerate(columns)
    ]
    for copy in forwards:
        copy.start()
    for i, (dx, dz) in enumerate(OFFSETS):
        outgoing[1][i].wait_recv()
        source = peer(me, (SIDE - dx) % SIDE, (SIDE - dz) % SIDE)
        schur_out[source] = schur_out[source] + landed[source]
        if i == PEERS // 2:
            for copy in forwards:
                copy.wait()
            flat = jnp.sum(column_counts[...], axis=0)
            share_out[...] = jnp.sum(flat, axis=1, keepdims=True) / float(N_ROW * N_COL * S)
    for copy in outgoing[0]:
        copy.wait()
    for copy in outgoing[1]:
        copy.wait_send()
    for kind in incoming:
        for copy in kind:
            copy.wait_send()


def fronts(child_blocks, front_pivot, front_update, child_map):
    any_spec = pl.BlockSpec(memory_space=pl.ANY)
    vmem_spec = pl.BlockSpec(memory_space=pltpu.VMEM)
    dma = pltpu.SemaphoreType.DMA
    return pl.pallas_call(
        fronts_kernel,
        out_shape=(
            pltpu.VMEM((N_ROW, UP, S), F32),
            pltpu.VMEM((N_ROW, UP, U), F32),
            jax.ShapeDtypeStruct((1, 1), F32),
        ),
        in_specs=[any_spec] * 4,
        out_specs=(vmem_spec, vmem_spec, vmem_spec),
        scratch_shapes=[
            pltpu.VMEM((2, CU), jnp.int32),
            pltpu.VMEM((N_ROW, 2, HELD, 128), F32),
            pltpu.VMEM((N_ROW, HELD, 128), F32),
            pltpu.VMEM((N_ROW, 8, 128), F32),
            pltpu.VMEM((CU, 128), F32),
            pltpu.VMEM((N_ROW * 8, 128), F32),
            pltpu.VMEM((2, CU, 128), F32),
            pltpu.VMEM((CU, 128), F32),
            pltpu.VMEM((F, S), F32),
            pltpu.VMEM((2, F, CU), BF16),
            pltpu.VMEM((CU, CU), BF16),
            pltpu.VMEM((CU, CU), BF16),
            pltpu.VMEM((2, 2, F, CU), BF16),
            pltpu.VMEM((S, 2 * S), F32),
            pltpu.VMEM((U, S), F32),
            pltpu.VMEM((U, U), F32),
            pltpu.VMEM((U, S), F32),
            pltpu.VMEM((N_ROW, UP, U), F32),
            pltpu.VMEM((1, 1, S), F32),
            pltpu.VMEM((N_ROW, 1, S), F32),
            pltpu.VMEM((1, 1, S), F32),
            pltpu.VMEM((N_COL, 1, S), F32),
            dma((PIECES + 3,)),
            dma((PEERS, PIECES)),
            dma((PEERS, PIECES)),
            dma((PEERS, 2)),
            dma((PEERS, 2)),
            dma((N_COL - 1,)),
            dma((N_COL - 1,)),
            dma((PEERS,)),
            dma((PEERS,)),
        ],
        compiler_params=pltpu.CompilerParams(collective_id=0, has_side_effects=True),
        name="fronts",
    )(child_blocks, front_pivot, front_update, child_map)


def store_kernel(lhat_ref, schur_ref, lhat_out, schur_out, sem):
    copies = [pltpu.make_async_copy(lhat_ref, lhat_out, sem.at[N_ROW])]
    for i in range(N_ROW):
        copies.append(pltpu.make_async_copy(schur_ref.at[i], schur_out.at[i], sem.at[i]))
    for copy in copies:
        copy.start()
    for copy in copies:
        copy.wait()


def store(lhat, schur):
    any_spec = pl.BlockSpec(memory_space=pl.ANY)
    vmem_spec = pl.BlockSpec(memory_space=pltpu.VMEM)
    return pl.pallas_call(
        store_kernel,
        out_shape=(
            jax.ShapeDtypeStruct(lhat.shape, F32),
            jax.ShapeDtypeStruct(schur.shape, F32),
        ),
        in_specs=[vmem_spec] * 2,
        out_specs=(any_spec,) * 2,
        scratch_shapes=[pltpu.SemaphoreType.DMA((N_ROW + 1,))],
        compiler_params=pltpu.CompilerParams(vmem_limit_bytes=1 << 20),
        name="store",
    )(lhat, schur)


def local(front_pivot, front_update, child_blocks, child_map):
    lhat, schur, share = fronts(child_blocks, front_pivot, front_update, child_map)
    lhat, schur = store(lhat, schur)
    return (lhat, schur, share[0, 0])


def solution(mesh):
    in_specs = (
        P("col", "row", None),
        P("col", "row", None),
        P("col", None, "row", None),
        P("col", None, None),
    )
    out_specs = (P("col", "row", None), P("col", "row", None), P())
    return jax.shard_map(local, mesh=mesh, in_specs=in_specs, out_specs=out_specs, check_vma=False)
```

```python
import jax
import jax.numpy as jnp
from jax import lax
from jax.experimental import pallas as pl
from jax.experimental.pallas import tpu as pltpu
from jax.sharding import PartitionSpec as P

MESH = pl.DeviceIdType.MESH
F32 = jnp.float32
BF16 = jnp.bfloat16
HIGHEST = lax.Precision.HIGHEST

N_ROW = 16
N_COL = 8
SIDE = 4
S = 128
CU = 512
U = 640
F = 768
SP = 8
UP = 40
HELD = 32
BLOCK = 64
ALL = [(dx, (dx + t) % 4) for t in range(4) for dx in range(4) if (dx, (dx + t) % 4) != (0, 0)]
OFFSETS = ALL
PEERS = len(OFFSETS)
PIECES = 7


def peer(me, dx, dz):
    x = lax.rem(me // SIDE + dx, SIDE)
    z = lax.rem(lax.rem(me, SIDE) + dz, SIDE)
    return x * SIDE + z


def to_row(source, target, send_sem, recv_sem, row):
    return pltpu.make_async_remote_copy(
        src_ref=source,
        dst_ref=target,
        send_sem=send_sem,
        recv_sem=recv_sem,
        device_id={"row": row},
        device_id_type=MESH,
    )


def split(values):
    high = values.astype(BF16)
    low = (values - high.astype(F32)).astype(BF16)
    return high, low


def nt_dot(a, b, precision=None):
    return lax.dot_general(
        a, b, (((1,), (1,)), ((), ())), precision=precision, preferred_element_type=F32
    )


def spread_lane(values, lane):
    return jnp.broadcast_to(values[:, lane : lane + 1], (8, 128))


def spread_row(values, row):
    return jnp.broadcast_to(values[row : row + 1, :], (8, 128))


def factor_in_place(work, meanwhile):
    sub = lax.broadcasted_iota(jnp.int32, (8, 128), 0)
    groups = BLOCK // 8
    for block in range(S // BLOCK):
        base = block * BLOCK
        left = [work[base + 8 * g : base + 8 * g + 8, 0:128] for g in range(groups)]
        right = [work[base + 8 * g : base + 8 * g + 8, 128:256] for g in range(groups)]
        inverted = []
        for panel in range(groups):
            scales = jnp.zeros((8, 128), F32)
            active = range(panel, groups)
            columns = [
                {g: spread_lane(left[g], base + 8 * panel + j) for g in active} for j in range(8)
            ]
            for j in range(0, 8, 2):
                first, second = columns[j], columns[j + 1]
                corner = spread_row(first[panel], j)
                side = spread_row(first[panel], j + 1)
                top = spread_row(second[panel], j)
                determinant = corner * spread_row(second[panel], j + 1) - side * top
                scale = 1.0 / corner
                next_scale = corner * (1.0 / determinant)
                ratio = side * scale
                scales = jnp.where(sub == j, scale, scales)
                scales = jnp.where(sub == j + 1, next_scale, scales)
                row_left = spread_row(left[panel], j)
                row_right = spread_row(right[panel], j)
                next_left = spread_row(left[panel], j + 1) - ratio * row_left
                next_right = spread_row(right[panel], j + 1) - ratio * row_right
                across = {i: spread_row(columns[i][panel], j) for i in range(j + 2, 8)}
                next_across = {
                    i: spread_row(columns[i][panel], j + 1) - ratio * across[i] for i in range(j + 2, 8)
                }
                for g in active:
                    multiplier = first[g] * scale
                    if g == panel:
                        multiplier = jnp.where(sub > j, multiplier, 0.0)
                    next_multiplier = (second[g] - multiplier * top) * next_scale
                    if g == panel:
                        next_multiplier = jnp.where(sub > j + 1, next_multiplier, 0.0)
                    for i in range(j + 2, 8):
                        columns[i][g] = (columns[i][g] - multiplier * across[i]) - next_multiplier * next_across[i]
                    left[g] = (left[g] - multiplier * row_left) - next_multiplier * next_left
                    right[g] = (right[g] - multiplier * row_right) - next_multiplier * next_right
            inverted.append(scales)
            if meanwhile and panel % 2 == 0:
                meanwhile.pop(0)()
        strip_left = jnp.concatenate(left, axis=0)
        strip_right = jnp.concatenate(right, axis=0)
        work[base : base + BLOCK, 0:128] = strip_left
        work[base : base + BLOCK, 128:256] = strip_right
        after = base + BLOCK
        if after < S:
            lower = strip_left * jnp.concatenate(inverted, axis=0)
            strip = jnp.concatenate([strip_left, strip_right], axis=1)
            product = lax.dot_general(
                lower, strip, (((0,), (0,)), ((), ())), precision=HIGHEST, preferred_element_type=F32
            )
            work[after:S, :] = work[after:S, :] - product[after:S, :]
    while meanwhile:
        meanwhile.pop(0)()


def turned(values, shift):
    shift %= 128
    if shift == 0:
        return values
    return jnp.concatenate([values[:, 128 - shift :], values[:, : 128 - shift]], axis=1)


def pack(near_src, packed_src, extra_src, quarter):
    which = jnp.full((HELD, 128), quarter, jnp.int32)
    lane = lax.broadcasted_iota(jnp.int32, (HELD, 128), 1)

    def one(front, carry):
        aligned = []
        for child in range(2):
            strip = near_src[front, child]
            result = strip
            for q in range(1, 4):
                result = jnp.where(which == q, turned(strip, -32 * q), result)
            aligned.append(result)
        packed_src[front] = jnp.where(lane < 64, aligned[0], turned(aligned[1], 64))
        chosen = jnp.where(which < 2, aligned[0], aligned[1])
        extra = turned(chosen[0:8], -64)
        for q in range(1, 4):
            moved = turned(chosen[8 * q : 8 * q + 8], 32 * q - 64)
            extra = jnp.where(lane[0:8] // 32 == q, moved, extra)
        extra_src[front] = extra
        return carry

    lax.fori_loop(0, N_ROW, one, 0)


def unpack(near_ref, extra_ref, child, group):
    lane = lax.broadcasted_iota(jnp.int32, (8, 128), 1) // 32
    rows = []
    for s in range(4):
        source = 4 * group + s
        strip = near_ref[32 * source : 32 * source + 32, :]
        strip = turned(strip, 32 * s - 64 * child)
        if s // 2 == child:
            extra = extra_ref[8 * source : 8 * source + 8, :]
            for q in range(4):
                moved = turned(extra, 32 * ((s + 2) % 4) - 32 * q)
                rows.append(jnp.where(lane == (s + 2) % 4, moved, strip[8 * q : 8 * q + 8]))
        else:
            rows.append(strip)
    half = jnp.concatenate(rows, axis=0)
    above = lax.broadcasted_iota(jnp.int32, (128, 128), 0) // 32
    ahead = (lax.broadcasted_iota(jnp.int32, (128, 128), 1) // 32 - above + 4) % 4
    kept = (ahead < 2) | ((ahead == 2) & (above // 2 == child))
    return jnp.where(kept, half, half.T)


def fronts_kernel(
    child_ref, pivot_ref, update_ref, map_ref, lhat_out, schur_out, share_out,
    maps, near_src, packed_src, extra_src, near_ref, extra_ref, next_ref, far_ref, panel_ref, hot_ref, high_ref, low_ref, spread_ref, work,
    lhat_ref, rest_ref, added_ref, landed, negative_ref, row_counts, total_ref, column_counts,
    own_sem, in_send, in_recv, out_send, out_recv, count_send, count_recv, row_send, row_recv,
):
    me = lax.axis_index("row")
    col = lax.axis_index("col")
    others = [peer(me, dx, dz) for dx, dz in OFFSETS]
    columns = [lax.rem(col + d, N_COL) for d in range(1, N_COL)]

    barrier = pltpu.get_barrier_semaphore()
    for other in others:
        pl.semaphore_signal(barrier, inc=1, device_id={"row": other}, device_id_type=MESH)
    for other in columns:
        pl.semaphore_signal(barrier, inc=1, device_id={"col": other}, device_id_type=MESH)

    group = me // SIDE
    near = pl.multiple_of(group * 128, 128)
    following = pl.multiple_of(lax.rem(group + 1, 4) * 128, 128)
    opposite = pl.multiple_of(lax.rem(group + 2, 4) * 128, 128)
    far_child = group // 2
    held = pl.ds(pl.multiple_of(me * HELD, HELD), HELD)
    pivot_rows = pl.ds(pl.multiple_of(me * SP, SP), SP)
    update_rows = pl.ds(pl.multiple_of(S + me * UP, SP), UP)

    extra_rows = pl.ds(pl.multiple_of(me * 8, 8), 8)

    def pieces(front):
        return (
            (pivot_ref.at[front], panel_ref.at[pivot_rows]),
            (packed_src.at[front], near_ref.at[held]),
            (extra_src.at[front], extra_ref.at[extra_rows]),
            (child_ref.at[front, 0, :, pl.ds(following, 128)], next_ref.at[0, held]),
            (child_ref.at[front, far_child, :, pl.ds(opposite, 128)], far_ref.at[held]),
            (child_ref.at[front, 1, :, pl.ds(following, 128)], next_ref.at[1, held]),
            (update_ref.at[front, :, pl.ds(0, S)], panel_ref.at[update_rows]),
        )

    near_copy = pltpu.make_async_copy(
        child_ref.at[:, :, :, pl.ds(near, 128)], near_src, own_sem.at[PIECES + 2]
    )
    near_copy.start()
    map_copy = pltpu.make_async_copy(map_ref.at[me], maps, own_sem.at[PIECES])
    map_copy.start()
    own = [
        pltpu.make_async_copy(source, target, own_sem.at[i])
        for i, (source, target) in enumerate(pieces(me))
    ]
    near_copy.wait()
    pack(near_src, packed_src, extra_src, lax.rem(me, 4))
    for copy in own:
        copy.start()
    pl.semaphore_wait(barrier, PEERS + N_COL - 1)
    incoming = [
        [
            to_row(*pieces(other)[i], in_send.at[place, i], in_recv.at[place, i], other)
            for place, other in enumerate(others)
        ]
        for i in range(PIECES)
    ]
    for kind in incoming:
        for copy in kind:
            copy.start()

    def arrived(kinds):
        for i in kinds:
            own[i].wait()
            for copy in incoming[i]:
                copy.wait_recv()

    trailing_copy = pltpu.make_async_copy(
        update_ref.at[:, :, pl.ds(S, U)], schur_out, own_sem.at[PIECES + 1]
    )
    trailing_copy.start()
    map_copy.wait()
    for child in range(2):
        indices = maps[child : child + 1, :]
        position = lax.broadcasted_iota(jnp.int32, (F, CU), 0)
        hot_ref[child] = jnp.where(indices == position, 1.0, 0.0).astype(BF16)

    def fill(i, j, block):
        high, low = split(block)
        high_ref[128 * i : 128 * i + 128, 128 * j : 128 * j + 128] = high
        low_ref[128 * i : 128 * i + 128, 128 * j : 128 * j + 128] = low

    def fill_near(child):
        for i in range(4):
            fill(i, i, unpack(near_ref, extra_ref, child, i))

    def fill_child(child):
        for i in range(4):
            rows = slice(128 * i, 128 * i + 128)
            block = next_ref[child, rows, :]
            fill(i, (i + 1) % 4, block)
            fill((i + 1) % 4, i, block.T)
        for i in (2 * child, 2 * child + 1):
            block = far_ref[128 * i : 128 * i + 128, :]
            fill(i, (i + 2) % 4, block)
            fill((i + 2) % 4, i, block.T)

    def spread_rows(child, first, count):
        for part, ref in enumerate((high_ref, low_ref)):
            spread_ref[child, part, first : first + count, :] = jnp.dot(
                hot_ref[child, first : first + count, :], ref[...], preferred_element_type=F32
            ).astype(BF16)

    def placed(start, size, first, count):
        total = None
        for child in range(2):
            hot = hot_ref[child, start : start + size, :]
            for part in range(2):
                term = nt_dot(spread_ref[child, part, first : first + count, :], hot)
                total = term if total is None else total + term
        return total

    arrived((0, 1, 2, 3, 4))
    fill_near(0)
    fill_child(0)
    spread_rows(0, 0, F)
    fill_near(1)
    arrived((5,))
    fill_child(1)
    spread_rows(1, 0, S)
    lane = lax.broadcasted_iota(jnp.int32, (S, S), 1)
    place = lax.broadcasted_iota(jnp.int32, (S, S), 0)
    work[:, 0:128] = panel_ref[0:S, :] + placed(0, S, 0, S)
    work[:, 128:256] = jnp.where(lane == place, 1.0, 0.0)

    def spread_later(first):
        return lambda: spread_rows(1, first, 320)

    def placed_later(start, first):
        def run():
            block = placed(start, 256, first, 320)
            rows = slice(first - S, first - S + 320)
            if start == 0:
                added_ref[rows, :] = block[:, 0:128]
                rest_ref[rows, 0:128] = block[:, 128:256]
            else:
                rest_ref[rows, start - S : start - S + 256] = block
        return run

    halves = (S, S + 320)
    factor_in_place(
        work,
        [spread_later(first) for first in halves]
        + [placed_later(start, first) for start in (0, 256, 512) for first in halves],
    )
    inverse = work[:, 128:256]
    pivots = jnp.sum(jnp.where(lane == place, work[:, 0:128], 0.0), axis=0, keepdims=True)
    negative = jnp.where(pivots < 0.0, 1.0, 0.0)
    negative_ref[0] = negative
    row_counts[me] = negative
    tallies = [
        to_row(negative_ref.at[0], row_counts.at[me], row_send.at[i], row_recv.at[i], other)
        for i, other in enumerate(others)
    ]
    for copy in tallies:
        copy.start()
    arrived((6,))
    lhat = nt_dot(panel_ref[S:, :] + added_ref[...], inverse, HIGHEST)
    lhat_ref[...] = lhat

    def share(row):
        return pl.ds(pl.multiple_of(row * UP, SP), UP)

    outgoing = [
        [
            to_row(
                source.at[share(other)], target.at[me], out_send.at[i, kind], out_recv.at[i, kind], other
            )
            for i, other in enumerate(others)
        ]
        for kind, (source, target) in enumerate(((lhat_ref, lhat_out), (rest_ref, landed)))
    ]
    for copy in outgoing[0]:
        copy.start()
    lhat_high, lhat_low = split(lhat)
    scaled_high, scaled_low = split(lhat / pivots)
    scaled_both = jnp.concatenate([scaled_high, scaled_low], axis=1)
    lhat_twice = jnp.concatenate([lhat_high, lhat_high], axis=1)
    for start, size in ((0, 256), (256, 256), (512, 128)):
        part = slice(start, start + size)
        correction = nt_dot(scaled_both, lhat_twice[part]) + nt_dot(scaled_high, lhat_low[part])
        rest_ref[:, start : start + size] = rest_ref[:, start : start + size] - correction
    for copy in outgoing[1]:
        copy.start()
    lhat_out[me] = lhat_ref[share(me), :]
    for copy in tallies:
        copy.wait()
    row_total = jnp.sum(row_counts[...], axis=0)
    total_ref[0] = row_total
    column_counts[col] = row_total
    trailing_copy.wait()
    schur_out[me] = schur_out[me] + rest_ref[share(me), :]
    forwards = [
        pltpu.make_async_remote_copy(
            src_ref=total_ref.at[0],
            dst_ref=column_counts.at[col],
            send_sem=count_send.at[i],
            recv_sem=count_recv.at[i],
            device_id={"col": other},
            device_id_type=MESH,
        )
        for i, other in enumerate(columns)
    ]
    for copy in forwards:
        copy.start()
    for i, (dx, dz) in enumerate(OFFSETS):
        outgoing[1][i].wait_recv()
        source = peer(me, (SIDE - dx) % SIDE, (SIDE - dz) % SIDE)
        schur_out[source] = schur_out[source] + landed[source]
        if i == PEERS // 2:
            for copy in forwards:
                copy.wait()
            flat = jnp.sum(column_counts[...], axis=0)
            share_out[...] = jnp.sum(flat, axis=1, keepdims=True) / float(N_ROW * N_COL * S)
    for copy in outgoing[0]:
        copy.wait()
    for copy in outgoing[1]:
        copy.wait_send()
    for kind in incoming:
        for copy in kind:
            copy.wait_send()


def fronts(child_blocks, front_pivot, front_update, child_map):
    any_spec = pl.BlockSpec(memory_space=pl.ANY)
    vmem_spec = pl.BlockSpec(memory_space=pltpu.VMEM)
    dma = pltpu.SemaphoreType.DMA
    return pl.pallas_call(
        fronts_kernel,
        out_shape=(
            pltpu.VMEM((N_ROW, UP, S), F32),
            pltpu.VMEM((N_ROW, UP, U), F32),
            jax.ShapeDtypeStruct((1, 1), F32),
        ),
        in_specs=[any_spec] * 4,
        out_specs=(vmem_spec, vmem_spec, vmem_spec),
        scratch_shapes=[
            pltpu.VMEM((2, CU), jnp.int32),
            pltpu.VMEM((N_ROW, 2, HELD, 128), F32),
            pltpu.VMEM((N_ROW, HELD, 128), F32),
            pltpu.VMEM((N_ROW, 8, 128), F32),
            pltpu.VMEM((CU, 128), F32),
            pltpu.VMEM((N_ROW * 8, 128), F32),
            pltpu.VMEM((2, CU, 128), F32),
            pltpu.VMEM((CU, 128), F32),
            pltpu.VMEM((F, S), F32),
            pltpu.VMEM((2, F, CU), BF16),
            pltpu.VMEM((CU, CU), BF16),
            pltpu.VMEM((CU, CU), BF16),
            pltpu.VMEM((2, 2, F, CU), BF16),
            pltpu.VMEM((S, 2 * S), F32),
            pltpu.VMEM((U, S), F32),
            pltpu.VMEM((U, U), F32),
            pltpu.VMEM((U, S), F32),
            pltpu.VMEM((N_ROW, UP, U), F32),
            pltpu.VMEM((1, 1, S), F32),
            pltpu.VMEM((N_ROW, 1, S), F32),
            pltpu.VMEM((1, 1, S), F32),
            pltpu.VMEM((N_COL, 1, S), F32),
            dma((PIECES + 3,)),
            dma((PEERS, PIECES)),
            dma((PEERS, PIECES)),
            dma((PEERS, 2)),
            dma((PEERS, 2)),
            dma((N_COL - 1,)),
            dma((N_COL - 1,)),
            dma((PEERS,)),
            dma((PEERS,)),
        ],
        compiler_params=pltpu.CompilerParams(collective_id=0, has_side_effects=True),
        name="fronts",
    )(child_blocks, front_pivot, front_update, child_map)


def store_kernel(lhat_ref, schur_ref, lhat_out, schur_out, sem):
    copies = [pltpu.make_async_copy(lhat_ref, lhat_out, sem.at[N_ROW])]
    for i in range(N_ROW):
        copies.append(pltpu.make_async_copy(schur_ref.at[i], schur_out.at[i], sem.at[i]))
    for copy in copies:
        copy.start()
    for copy in copies:
        copy.wait()


def store(lhat, schur):
    any_spec = pl.BlockSpec(memory_space=pl.ANY)
    vmem_spec = pl.BlockSpec(memory_space=pltpu.VMEM)
    return pl.pallas_call(
        store_kernel,
        out_shape=(
            jax.ShapeDtypeStruct(lhat.shape, F32),
            jax.ShapeDtypeStruct(schur.shape, F32),
        ),
        in_specs=[vmem_spec] * 2,
        out_specs=(any_spec,) * 2,
        scratch_shapes=[pltpu.SemaphoreType.DMA((N_ROW + 1,))],
        compiler_params=pltpu.CompilerParams(vmem_limit_bytes=1 << 20),
        name="store",
    )(lhat, schur)


def local(front_pivot, front_update, child_blocks, child_map):
    lhat, schur, share = fronts(child_blocks, front_pivot, front_update, child_map)
    lhat, schur = store(lhat, schur)
    return (lhat, schur, share[0, 0])


def solution(mesh):
    in_specs = (
        P("col", "row", None),
        P("col", "row", None),
        P("col", None, "row", None),
        P("col", None, None),
    )
    out_specs = (P("col", "row", None), P("col", "row", None), P())
    return jax.shard_map(local, mesh=mesh, in_specs=in_specs, out_specs=out_specs, check_vma=False)
```
